32 devices in a mesh: lat: 4 (over y, x), lon: 8 (over z, core).
Axes of the slice: x: 2, y: 2, z: 4, core: 2. Of those that a mesh axis runs over, the one named last changes fastest.
Arguments:
- forcing: float32 [256, 2048], P('lat', 'lon'), may hold values from -32 to 32
- depth_east: float32 [256, 2048], P('lat', 'lon'), may hold values from 0.25 to 4
- depth_north: float32 [256, 2048], P('lat', 'lon'), may hold values from 0.25 to 4
- surface_term: float32 [256, 2048], P('lat', 'lon'), may hold values from 0.02 to 0.5
- ocean_mask: int32 [256, 2048], P('lat', 'lon'), may hold values 0 or 1
- cost_weights: float32 [8, 256, 2048], P(None, 'lat', 'lon'), may hold values from -6 to 6
Outputs:
- forcing_adjoint: float32 [8, 256, 2048], P(None, 'lat', 'lon')
- east_gradient: float32 [8, 256, 2048], P(None, 'lat', 'lon')
- north_gradient: float32 [8, 256, 2048], P(None, 'lat', 'lon')
The draws below stay inside these ranges and needn't reach their ends.
Inputs may be any that keep to these rules, and one draw needn't show every extreme that they name: `ocean_mask`: 1 marks an ocean cell, 0 a land cell.
All inputs are finite; a program needn't handle non-finite values. No bound on the sum of `ocean_mask` on one device may be relied on, other than what follows from the above.
Results may differ from the reference program's by a relative error of at most 0.00018.
Values sent between devices are 32-bit elements; how exact they have to be, the bound alone decides.
A program may use at most 64 MiB of HBM per device.

```python
import math
import jax
import jax.numpy as jnp
from jax import lax

COSTS = 8
ITERS = 6
NLAT = 256
NLON = 2048


def draw_forcing(key, part):
    first = jax.random.fold_in(key, 0)
    rows = jnp.arange(NLAT, dtype=jnp.float32) / NLAT
    cols = jnp.arange(NLON, dtype=jnp.float32) / NLON
    envelope = jnp.exp(jnp.log(3.0) * (0.5 * rows[:, None] + cols[None, :]))
    rough = jnp.clip(jax.random.normal(first, (NLAT, NLON), jnp.float32), -6.0, 6.0)
    return (rough * envelope).astype(jnp.float32)


def plant(values, key, least, high):
    index_at = [jax.random.randint(jax.random.fold_in(key, axis), (), 0, length) for axis, length in enumerate(values.shape)]
    longest = values.shape.index(max(values.shape))
    beside = index_at[:longest] + [(index_at[longest] + 1) % values.shape[longest]] + index_at[longest + 1:]
    return values.at[tuple(index_at)].set(least).at[tuple(beside)].set(high)


def block_scale(own_key, extent, shards, smallest, top_value):
    def one(dim, shards_of):
        heights = jax.random.uniform(jax.random.fold_in(jax.random.fold_in(own_key, 6), dim), (shards_of,), jnp.float32, smallest / len(shards), top_value / len(shards))
        return jnp.repeat(jnp.exp(heights), extent[dim] // shards_of).reshape((-1,) + (1,) * (len(extent) - dim - 1))

    level = one(*shards[0])
    for cut in shards[1:]:
        level = level * one(*cut)
    return level


def scatter_about(key, shape, scale, reach, shards=(), held_as=jnp.bfloat16):
    entries = scale * jax.random.normal(key, shape, jnp.float32)
    if shards:
        entries = entries * block_scale(key, shape, shards, -0.22, 0.18)
    return jnp.clip(entries, -reach, reach).astype(held_as)


def setup_inputs(seed: int = 0) -> dict:
    keys = jax.random.split(jax.random.key(seed), 7)
    forcing = draw_forcing(jax.random.fold_in(keys[6], 71), 0)
    depth_east = jnp.clip(jnp.exp(math.log(4.0) - 2.7725887 * jax.random.uniform(keys[1], (NLAT, NLON), jnp.float32) ** block_scale(keys[1], (NLAT, NLON), ((0, 4), (1, 8)), -0.2, 0.2)), 0.25, 4.0)
    depth_north = jnp.clip(jnp.exp(math.log(4.0) - 2.7725887 * jax.random.uniform(keys[2], (NLAT, NLON), jnp.float32) ** block_scale(keys[2], (NLAT, NLON), ((0, 4), (1, 8)), -0.2, 0.2)), 0.25, 4.0)
    surface_term = jnp.clip(jnp.exp(math.log(0.5) - 3.218876 * jax.random.uniform(keys[3], (NLAT, NLON), jnp.float32) ** block_scale(keys[3], (NLAT, NLON), ((0, 4), (1, 8)), -0.2, 0.2)), 0.02, 0.5)
    ocean_mask = plant((jax.random.randint(keys[4], (NLAT, NLON), 0, 5) < 4).astype(jnp.int32), jax.random.fold_in(keys[4], 1), 0, 1)
    cost_weights = scatter_about(keys[5], (COSTS, NLAT, NLON), 1.0, 6.0, ((1, 4), (2, 8)), jnp.float32)
    return {"forcing": forcing, "depth_east": depth_east, "depth_north": depth_north, "surface_term": surface_term, "ocean_mask": ocean_mask, "cost_weights": cost_weights}


def faces(ocean_mask, depth_east, depth_north, surface_term):
    wet = ocean_mask.astype(jnp.float32)
    wet_east = jnp.roll(wet, -1, axis=1)
    wet_north = jnp.concatenate([wet[1:], jnp.zeros((1, wet.shape[1]), jnp.float32)], axis=0)
    east_face = depth_east * wet * wet_east
    north_face = depth_north * wet * wet_north
    west_face = jnp.roll(east_face, 1, axis=1)
    south_face = jnp.concatenate([jnp.zeros((1, wet.shape[1]), jnp.float32), north_face[:-1]], axis=0)
    base = wet * surface_term + 1.0 - wet
    return (base, east_face, west_face, north_face, south_face)

def operate(field, coefs):
    base, east_face, west_face, north_face, south_face = coefs
    east = jnp.roll(field, -1, axis=1)
    west = jnp.roll(field, 1, axis=1)
    zero_row = jnp.zeros((1, field.shape[1]), jnp.float32)
    north = jnp.concatenate([field[1:], zero_row], axis=0)
    south = jnp.concatenate([zero_row, field[:-1]], axis=0)
    return base * field + east_face * (field - east) + west_face * (field - west) + north_face * (field - north) + south_face * (field - south)

def solve(forcing, depth_east, depth_north, surface_term, ocean_mask):
    coefs = faces(ocean_mask, depth_east, depth_north, surface_term)
    diagonal = coefs[0] + coefs[1] + coefs[2] + coefs[3] + coefs[4]
    iterate = jnp.zeros_like(forcing)
    residual = forcing
    precond = residual / diagonal
    direction = precond
    norm_now = jnp.sum(residual * precond)
    for step in range(ITERS):
        image = operate(direction, coefs)
        alpha = norm_now / jnp.sum(direction * image)
        iterate = iterate + alpha * direction
        residual = residual - alpha * image
        if step < ITERS - 1:
            precond = residual / diagonal
            norm_next = jnp.sum(residual * precond)
            direction = precond + norm_next / norm_now * direction
            norm_now = norm_next
    return iterate

def reference(forcing, depth_east, depth_north, surface_term, ocean_mask, cost_weights):

    def forward(rhs_field, east_depth, north_depth):
        return solve(rhs_field, east_depth, north_depth, surface_term, ocean_mask)
    _, pullback = jax.vjp(forward, forcing, depth_east, depth_north)
    grads = lax.map(lambda weight: pullback(weight), cost_weights)
    return (grads[0], grads[1], grads[2])
```

```python
import functools

import jax
import jax.numpy as jnp
from jax import lax
from jax.experimental import pallas as pl
from jax.experimental.pallas import tpu as pltpu
from jax.sharding import PartitionSpec as P

ITERS = 6
MESH = pl.DeviceIdType.MESH
HR = 16
HB = 8
HC = 13
HW = 6


def cost_of(mu, proj):
    def dot(a, b):
        acc = [None] * (len(a) + len(b) - 1)
        for i, x in enumerate(a):
            for j, y in enumerate(b):
                if a is b and j < i:
                    continue
                pr = x * y
                if a is b and j > i:
                    pr = pr + pr
                for m in (i + j, abs(i - j)):
                    acc[m] = pr if acc[m] is None else acc[m] + pr
        tot = acc[0] * mu[0]
        for m in range(1, len(acc)):
            tot = tot + acc[m] * mu[m]
        return 0.5 * tot

    def apply(p):
        q = list(p) + [None]
        for k, x in enumerate(p):
            if k == 0:
                q[1] = -x if q[1] is None else q[1] - x
            else:
                hx = 0.5 * x
                q[k + 1] = -hx if q[k + 1] is None else q[k + 1] - hx
                q[k - 1] = q[k - 1] - hx
        return q

    one = jnp.ones_like(mu[0])
    z, p, rz, cost = [one], [one], mu[0], None
    for step in range(ITERS):
        q = apply(p)
        alpha = rz / dot(p, q)
        term = p[0] * proj[0]
        for k in range(1, len(p)):
            term = term + p[k] * proj[k]
        cost = alpha * term if cost is None else cost + alpha * term
        if step < ITERS - 1:
            z = [z[k] - alpha * q[k] for k in range(len(z))] + [-alpha * q[-1]]
            rz_new = dot(z, z)
            beta = rz_new / rz
            p = [z[k] + beta * p[k] for k in range(len(p))] + [z[-1]]
            rz = rz_new
    return cost


def roll(x, shift, axis):
    return pltpu.roll(x, shift % x.shape[axis], axis)


def east(x):
    return roll(x, -1, 1)


def north(x):
    return roll(x, -1, 0)


def kernel(nlat, nlon, stages, f_hbm, de_hbm, dn_hbm, st_hbm, mk_hbm, w_hbm, wp, pack, geo, coef,
           f_ref, de_ref, dn_ref, st_ref, mk_ref, w_ref, lsem,
           send_w, send_e, recv_e, recv_w, row_n, row_s, mrow_n, mrow_s, wrow_n, wrow_s,
           sums, ssem, rsem, *reduce_refs):
    lat, lon = lax.axis_index("lat"), lax.axis_index("lon")
    costs, rows, cols = w_ref.shape
    loads = [pltpu.make_async_copy(src, dst, lsem.at[i]) for i, (src, dst) in enumerate(
        zip((f_hbm, de_hbm, dn_hbm, st_hbm, mk_hbm, w_hbm),
            (f_ref, de_ref, dn_ref, st_ref, mk_ref, w_ref)))]
    for c in loads:
        c.start()

    def peer(dlat, dlon):
        return (lax.rem(lat + dlat + nlat, nlat), lax.rem(lon + dlon + nlon, nlon))

    peers = {(a % nlat, b % nlon) for a in (-1, 0, 1) for b in (-1, 0, 1)}
    peers |= {o for stage in stages for o in stage}
    peers = sorted(peers - {(0, 0)})
    barrier = pltpu.get_barrier_semaphore()
    for a, b in peers:
        pl.semaphore_signal(barrier, inc=1, device_id=peer(a, b), device_id_type=MESH)

    for c in loads:
        c.wait()

    lane = lax.broadcasted_iota(jnp.int32, (rows, 128), 1)
    wide = [f_ref, de_ref, dn_ref, st_ref, mk_ref]
    for ref, at, first in ((send_w, slice(0, 128), True), (send_e, slice(cols - 128, cols), False)):
        buf = jnp.zeros((rows, 128), jnp.float32)
        pos = 0
        for i in range(5 + costs):
            width = HC if i < 5 else HW
            tile = (wide[i][:, at] if i < 5 else w_ref[i - 5, :, at]).astype(jnp.float32)
            tile = roll(tile, pos if first else pos + width, 1)
            buf = jnp.where((lane >= pos) & (lane < pos + width), tile, buf)
            pos += width
        ref[...] = buf
    pl.semaphore_wait(barrier, len(peers))

    copies = []

    def send(src, dst, dev):
        i = len(copies)
        c = pltpu.make_async_remote_copy(src_ref=src, dst_ref=dst, send_sem=ssem.at[i],
                                         recv_sem=rsem.at[i], device_id=dev, device_id_type=MESH)
        c.start()
        copies.append(c)

    lo, hi = pl.ds(0, HR), pl.ds(rows - HR, HR)
    for src, dst, d in ((send_w, recv_e, -1), (send_e, recv_w, 1)):
        send(src.at[lo], dst.at[pl.ds(rows, HR)], peer(-1, d))
        send(src.at[hi], dst.at[pl.ds(rows + HR, HR)], peer(1, d))
        send(src, dst.at[pl.ds(0, rows)], peer(0, d))
    for i in range(5):
        src = wide[i]
        send(src.at[lo], row_n.at[i] if i < 4 else mrow_n, peer(-1, 0))
        send(src.at[hi], row_s.at[i] if i < 4 else mrow_s, peer(1, 0))
    early = len(copies)
    send(w_ref.at[:, pl.ds(0, HB)], wrow_n, peer(-1, 0))
    send(w_ref.at[:, pl.ds(rows - HB, HB)], wrow_s, peer(1, 0))
    for c in copies[:early]:
        c.wait_recv()

    full = rows + 2 * HR
    lane = lax.broadcasted_iota(jnp.int32, (full, 128), 1)
    got_e, got_w = recv_e[...], recv_w[...]

    def side(pos, width):
        a = roll(got_e, -pos, 1)
        b = roll(got_w, 128 - width - pos, 1)
        return jnp.where(lane < width, a, jnp.where(lane >= 128 - width, b, 0.0))

    def padded(i):
        if i < 4:
            top, mid, low = row_n[i], wide[i][...], row_s[i]
        else:
            top, mid, low = (r[...].astype(jnp.float32) for r in (mrow_n, mk_ref, mrow_s))
        return jnp.concatenate([jnp.concatenate([mid, top, low], axis=0), side(HC * i, HC)], axis=1)

    ringc = cols + 128
    row_id = lax.broadcasted_iota(jnp.int32, (full, ringc), 0)
    keep_n = (lat < nlat - 1).astype(jnp.float32)
    keep_s = (lat > 0).astype(jnp.float32)
    edge = jnp.where(row_id < rows, 1.0, jnp.where(row_id < rows + HR, keep_n, keep_s))
    wet = padded(4) * edge
    ex = padded(1) * wet * east(wet)
    ey = padded(2) * wet * north(wet)
    base = wet * padded(3) + 1.0 - wet
    diag = base + ex + roll(ex, 1, 1) + ey + roll(ey, 1, 0)
    rs = lax.rsqrt(diag)
    rs = rs * (1.5 - 0.5 * diag * rs * rs)
    rs_e, rs_n = rs * east(rs), rs * north(rs)
    e2 = 2.0 * ex * rs_e
    n2 = 2.0 * ey * rs_n

    def twice(v, e2, n2):
        return e2 * east(v) + roll(e2 * v, 1, 1) + n2 * north(v) + roll(n2 * v, 1, 0)

    us = [rs * padded(0)]
    us.append(0.5 * twice(us[0], e2, n2))
    for k in range(1, ITERS):
        us.append(twice(us[k], e2, n2) - us[k - 1])

    inner = [u[:rows, :cols] for u in us]
    rs_in = rs[:rows, :cols]

    def put(at, field):
        line = jnp.sum(field, axis=0, keepdims=True)
        tot = line[:, :128]
        for c in range(128, cols, 128):
            tot = tot + line[:, c:c + 128]
        sums[at:at + 1, :] = tot

    sums[...] = jnp.zeros_like(sums)
    mom = ITERS * costs
    for k in range(ITERS):
        put(mom + 2 * k, inner[k] * inner[k])
        put(mom + 2 * k + 1, inner[k] * inner[k + 1])
    for n in range(costs):
        wn = w_ref[n] * rs_in
        for k in range(ITERS):
            put(k * costs + n, wn * inner[k])
    nsum = sums.shape[0]
    lane_s = lax.broadcasted_iota(jnp.int32, (nsum, 128), 1)
    row_s_id = lax.broadcasted_iota(jnp.int32, (nsum, 128), 0)
    by_row = jnp.sum(sums[...], axis=1, keepdims=True)
    mine = jnp.sum(jnp.where(lane_s == row_s_id, by_row, 0.0), axis=0, keepdims=True)
    reduce_copies = []

    def start(stage, value):
        mailbox, got, ss, rv = reduce_refs[4 * stage:4 * stage + 4]
        mailbox[...] = value
        group = []
        for i, (a, b) in enumerate(stages[stage]):
            c = pltpu.make_async_remote_copy(src_ref=mailbox, dst_ref=got.at[i], send_sem=ss.at[i],
                                             recv_sem=rv.at[i], device_id=peer(a, b),
                                             device_id_type=MESH)
            c.start()
            group.append(c)
        reduce_copies.extend(group)
        return group

    def finish(stage, group, value):
        for c in group:
            c.wait_recv()
        for i in range(len(group)):
            value = value + reduce_refs[4 * stage + 1][i]
        return value

    group = start(0, mine)

    for c in copies[early:]:
        c.wait_recv()

    def cut(x):
        return jnp.concatenate([x[:rows + HB], x[full - HB:]], axis=0)

    rs_b = cut(rs)
    for n in range(costs):
        block = jnp.concatenate([w_ref[n], wrow_n[n], wrow_s[n]], axis=0)
        tile = cut(side(5 * HC + HW * n, HW))
        wp[n] = rs_b * jnp.concatenate([block, tile], axis=1)
    for k in range(ITERS + 1):
        pack[k] = cut(us[k])
    pack[ITERS + 1], pack[ITERS + 2], pack[ITERS + 3] = cut(e2), cut(n2), rs_b
    wet_in = wet[:rows, :cols]
    me = wet_in * east(wet)[:rows, :cols]
    mn = wet_in * north(wet)[:rows, :cols]
    geo[0], geo[1] = me, mn
    geo[2] = 2.0 * me * rs_e[:rows, :cols]
    geo[3] = 2.0 * mn * rs_n[:rows, :cols]
    total = finish(0, group, mine)
    for stage in range(1, len(stages)):
        total = finish(stage, start(stage, total), total)

    tot8 = jnp.broadcast_to(total, (costs, 128))
    lane8 = lax.broadcasted_iota(jnp.int32, (costs, 128), 1)
    sub8 = lax.broadcasted_iota(jnp.int32, (costs, 128), 0)

    def pick(index):
        return jnp.broadcast_to(
            jnp.sum(jnp.where(lane8 == index, tot8, 0.0), axis=1, keepdims=True), (costs, 128))

    proj = [pick(k * costs + sub8) for k in range(ITERS)]
    raw = [pick(mom + m) for m in range(2 * ITERS)]
    mu = [raw[0], raw[1]]
    for k in range(1, ITERS):
        mu += [2.0 * raw[2 * k] - raw[0], 2.0 * raw[2 * k + 1] - raw[1]]
    cost, pull = jax.vjp(cost_of, mu, proj)
    mu_bar, x = pull(jnp.ones_like(cost))
    even = [2.0 * mu_bar[2 * k] for k in range(ITERS)]
    odd = [2.0 * mu_bar[2 * k + 1] for k in range(ITERS)]
    even[0] = mu_bar[0] - 0.5 * sum(even[1:])
    odd[0] = mu_bar[1] - 0.5 * sum(odd[1:])
    for k in range(ITERS):
        coef[3 * k], coef[3 * k + 1], coef[3 * k + 2] = x[k], 2.0 * even[k], odd[k]
    for c in copies + reduce_copies:
        c.wait_send()


def adjoint_kernel(wp, pack, geo, coef, fa_hbm, ge_hbm, gn_hbm,
                   u_in, u_east, u_north, quad, fa_ref, ge_ref, gn_ref,
                   osem):
    costs, rows, cols = fa_ref.shape
    ringc = wp.shape[2]
    def results(n):
        return [pltpu.make_async_copy(src.at[n], dst.at[n], osem.at[i, n])
                for i, (src, dst) in enumerate(((fa_ref, fa_hbm), (ge_ref, ge_hbm), (gn_ref, gn_hbm)))]

    for k in range(ITERS):
        u = pack[k] if k else 0.5 * pack[0]
        u_in[k] = u[:rows, :cols]
        u_east[k] = east(u)[:rows, :cols]
        u_north[k] = north(u)[:rows, :cols]
        quad[k] = pack[k] + pack[k - 2] if k > 1 else pack[k]
    quad[ITERS] = 0.5 * pack[ITERS] + pack[ITERS - 2]

    def one(n, carry):
        def c(i):
            return jnp.concatenate([coef[i, pl.ds(n, 1), :]] * (ringc // 128), axis=1)

        wn = wp[n]
        ub = [pack.at[k] for k in range(ITERS + 1)]
        e2b, n2b = pack[ITERS + 1], pack[ITERS + 2]
        nxt = c(3 * ITERS - 1) * ub[ITERS - 1][...]
        nxt2 = None
        dd = nxt * quad[ITERS]
        eb = nb = du = None
        for k in range(ITERS - 1, -1, -1):
            le, ln = east(nxt), north(nxt)
            s2 = e2b * le + roll(e2b * nxt, 1, 1) + n2b * ln + roll(n2b * nxt, 1, 0)
            if k == 0:
                s2 = 0.5 * s2
            lin = nxt[:rows, :cols]
            ea = lin * u_east[k] + le[:rows, :cols] * u_in[k]
            na = lin * u_north[k] + ln[:rows, :cols] * u_in[k]
            eb = ea if eb is None else eb + ea
            nb = na if nb is None else nb + na
            seed = c(3 * k + 1) * ub[k][...] + c(3 * k + 2) * ub[k + 1][...]
            if k > 0:
                seed = seed + c(3 * k - 1) * ub[k - 1][...]
            lam = c(3 * k) * wn + seed + s2
            if nxt2 is not None:
                lam = lam - nxt2
            dd = dd + lam * quad[k]
            du = seed * ub[k][...] if du is None else du + seed * ub[k][...]
            nxt, nxt2 = lam, nxt
        rs = pack[ITERS + 3]
        fa_ref[n] = rs[:rows, :cols] * nxt[:rows, :cols]
        db = -(rs * rs) * (dd - 0.5 * du)
        db_in = db[:rows, :cols]
        ge_ref[n] = geo[2] * eb + geo[0] * (db_in + east(db)[:rows, :cols])
        gn_ref[n] = geo[3] * nb + geo[1] * (db_in + north(db)[:rows, :cols])
        for r in results(n):
            r.start()
        return carry

    lax.fori_loop(0, costs, one, 0)
    for n in range(costs):
        for r in results(n):
            r.wait()


def solution(mesh):
    nlat, nlon = mesh.shape["lat"], mesh.shape["lon"]

    def body(forcing, depth_east, depth_north, surface_term, ocean_mask, cost_weights):
        costs, rows, cols = cost_weights.shape
        full, ringc = rows + 2 * HR, cols + 128
        f32 = jnp.float32
        dma = pltpu.SemaphoreType.DMA
        nsum = -(-(ITERS * costs + 2 * ITERS) // 8) * 8
        every = [(a, b) for a in range(nlat) for b in range(nlon) if a or b]
        stages = [every] if len(every) < 64 else [
            [(0, b) for b in range(1, nlon)], [(a, 0) for a in range(1, nlat)]]
        reduce_scratch = [
            ref for g in stages for ref in (
                pltpu.VMEM((1, 128), f32), pltpu.VMEM((len(g), 1, 128), f32),
                dma((len(g),)), dma((len(g),)))]
        bf = rows + 2 * HB
        shapes = ((costs, bf, ringc), (ITERS + 4, bf, ringc), (4, rows, cols), (3 * ITERS, costs, 128))
        hbm = pl.BlockSpec(memory_space=pltpu.HBM)
        vmem = pl.BlockSpec(memory_space=pltpu.VMEM)
        mids = pl.pallas_call(
            functools.partial(kernel, nlat, nlon, stages),
            out_shape=[pltpu.VMEM(x, f32) for x in shapes],
            in_specs=[hbm] * 6,
            out_specs=[vmem] * 4,
            scratch_shapes=[
                *[pltpu.VMEM((rows, cols), f32)] * 4,
                pltpu.VMEM((rows, cols), jnp.int32),
                pltpu.VMEM((costs, rows, cols), f32),
                dma((6,)),
                pltpu.VMEM((rows, 128), f32),
                pltpu.VMEM((rows, 128), f32),
                pltpu.VMEM((full, 128), f32),
                pltpu.VMEM((full, 128), f32),
                pltpu.VMEM((4, HR, cols), f32),
                pltpu.VMEM((4, HR, cols), f32),
                pltpu.VMEM((HR, cols), jnp.int32),
                pltpu.VMEM((HR, cols), jnp.int32),
                pltpu.VMEM((costs, HB, cols), f32),
                pltpu.VMEM((costs, HB, cols), f32),
                pltpu.VMEM((nsum, 128), f32),
                dma((18,)),
                dma((18,)),
                *reduce_scratch,
            ],
            compiler_params=pltpu.CompilerParams(
                collective_id=0, has_side_effects=True, vmem_limit_bytes=32 * 1024 * 1024
            ),
        )(*[pltpu.with_memory_space_constraint(x, pltpu.HBM) for x in (
            forcing, depth_east, depth_north, surface_term, ocean_mask, cost_weights)])
        out = (costs, rows, cols)
        return pl.pallas_call(
            adjoint_kernel,
            out_shape=[jax.ShapeDtypeStruct(out, f32)] * 3,
            in_specs=[vmem] * 4,
            out_specs=[hbm] * 3,
            scratch_shapes=[
                *[pltpu.VMEM((ITERS, rows, cols), f32)] * 3,
                pltpu.VMEM((ITERS + 1, bf, ringc), f32),
                *[pltpu.VMEM(out, f32)] * 3,
                dma((3, costs)),
            ],
            compiler_params=pltpu.CompilerParams(vmem_limit_bytes=32 * 1024 * 1024),
        )(*[pltpu.with_memory_space_constraint(x, pltpu.VMEM) for x in mids])

    grid = P("lat", "lon")
    field = P(None, "lat", "lon")
    return jax.shard_map(
        body,
        mesh=mesh,
        in_specs=(grid, grid, grid, grid, grid, field),
        out_specs=(field, field, field),
        check_vma=False,
    )
```

```python
import functools

import jax
import jax.numpy as jnp
from jax import lax
from jax.experimental import pallas as pl
from jax.experimental.pallas import tpu as pltpu
from jax.sharding import PartitionSpec as P

ITERS = 6
MESH = pl.DeviceIdType.MESH
HR = 16
HB = 8
HS = 5
BLOCK = 8
HC = 13
HW = 6
GROUP = 16
DEG = 2 * ITERS
CS, CC = 0, ITERS
CX = CC + ITERS
CH = CX + DEG - 1
CM = CH + DEG
NCOEF = CM + DEG


def coefficients(mu, proj):
    def gram(a, b):
        return 0.5 * (mu[a + b] + mu[abs(a - b)])

    h = {}
    for a in range(ITERS):
        for b in range(a, ITERS):
            h[a, b] = gram(a, b) - 0.5 * (gram(a, b + 1) + gram(a, abs(b - 1)))
    g, p = list(mu[:ITERS]), list(proj)
    low, inv = {}, []
    for i in range(ITERS):
        inv.append(1.0 / h[i, i])
        for j in range(i + 1, ITERS):
            low[j, i] = h[i, j] * inv[i]
        for j in range(i + 1, ITERS):
            for k in range(j, ITERS):
                h[j, k] = h[j, k] - low[j, i] * h[i, k]
            g[j] = g[j] - low[j, i] * g[i]
            p[j] = p[j] - low[j, i] * p[i]
    c, d = [None] * ITERS, [None] * ITERS
    for i in range(ITERS - 1, -1, -1):
        c[i], d[i] = g[i] * inv[i], p[i] * inv[i]
        for j in range(i + 1, ITERS):
            c[i] = c[i] - low[j, i] * c[j]
            d[i] = d[i] - low[j, i] * d[j]
    zero = jnp.zeros_like(c[0])
    cc = c + [zero, zero]
    res = [1.0 - c[0] + 0.5 * c[1], c[0] + 0.5 * cc[2] - c[1]]
    for j in range(2, ITERS + 1):
        res.append(0.5 * (cc[j - 1] + cc[j + 1]) - cc[j])
    bar = [zero] * DEG
    for a in range(ITERS):
        half = 0.5 * d[a]
        for j in range(ITERS + 1):
            t = half * res[j]
            bar[a + j] = bar[a + j] + t
            bar[abs(a - j)] = bar[abs(a - j)] + t
    return c, bar


def roll(x, shift, axis):
    return pltpu.roll(x, shift % x.shape[axis], axis)


def east(x):
    return roll(x, -1, 1)


def north(x):
    return roll(x, -1, 0)


def total_of(terms):
    acc = None
    for t in terms:
        acc = t if acc is None else acc + t
    return acc


def kernel(nlat, nlon, stages, f_hbm, de_hbm, dn_hbm, st_hbm, mk_hbm, w_hbm,
           un, ue, xe, xn, ww, v, ve, geo, dia, coef, us_side, vs_side,
           fields, mk_ref, w_ref, lsem,
           send_w, send_e, recv_e, recv_w, row_n, row_s, mrow_n, mrow_s, wrow_n, wrow_s,
           wsend_w, wsend_e, wrecv_e, wrecv_w, up, unn, e2r, n2r, rsr, comb, ssem, rsem, *reduce_refs):
    lat, lon = lax.axis_index("lat"), lax.axis_index("lon")
    rows, costs, cols = w_ref.shape
    for i, src in enumerate((f_hbm, de_hbm, dn_hbm, st_hbm)):
        pltpu.make_async_copy(src, fields.at[i], lsem.at[0]).start()
    pltpu.make_async_copy(mk_hbm, mk_ref, lsem.at[1]).start()
    for n in range(costs):
        pltpu.make_async_copy(w_hbm.at[n], w_ref.at[:, n, :], lsem.at[2]).start()

    def loaded(i, ref):
        pltpu.make_async_copy(ref, ref, lsem.at[i]).wait()

    def peer(dlat, dlon):
        return (lax.rem(lat + dlat + nlat, nlat), lax.rem(lon + dlon + nlon, nlon))

    peers = {(a % nlat, b % nlon) for a in (-1, 0, 1) for b in (-1, 0, 1)}
    peers |= {o for stage in stages for o in stage}
    peers = sorted(peers - {(0, 0)})
    barrier = pltpu.get_barrier_semaphore()
    for a, b in peers:
        pl.semaphore_signal(barrier, inc=1, device_id=peer(a, b), device_id_type=MESH)

    loaded(0, fields)
    loaded(1, mk_ref)

    lane = lax.broadcasted_iota(jnp.int32, (rows, 128), 1)
    wide = [fields.at[i] for i in range(4)] + [mk_ref]
    for ref, at, first in ((send_w, slice(0, 128), True), (send_e, slice(cols - 128, cols), False)):
        buf = jnp.zeros((rows, 128), jnp.float32)
        for i in range(5):
            pos = HC * i
            tile = wide[i][:, at].astype(jnp.float32)
            tile = roll(tile, pos if first else pos + HC, 1)
            buf = jnp.where((lane >= pos) & (lane < pos + HC), tile, buf)
        ref[...] = buf
    pl.semaphore_wait(barrier, len(peers))

    waits = []

    def send(whole, parts):
        i = len(waits)
        for src, dst, dev in parts:
            pltpu.make_async_remote_copy(src_ref=src, dst_ref=dst, send_sem=ssem.at[i], recv_sem=rsem.at[i],
                                         device_id=dev, device_id_type=MESH).start()
        waits.append(pltpu.make_async_remote_copy(src_ref=whole, dst_ref=whole, send_sem=ssem.at[i],
                                                  recv_sem=rsem.at[i], device_id=peer(0, 1), device_id_type=MESH))

    lo, hi = pl.ds(0, HR), pl.ds(rows - HR, HR)
    send(row_n, [(fields.at[:, lo], row_n, peer(-1, 0))])
    send(row_s, [(fields.at[:, hi], row_s, peer(1, 0))])
    send(mrow_n, [(mk_ref.at[lo], mrow_n, peer(-1, 0))])
    send(mrow_s, [(mk_ref.at[hi], mrow_s, peer(1, 0))])
    for src, dst, d in ((send_w, recv_e, -1), (send_e, recv_w, 1)):
        send(dst, [(src.at[lo], dst.at[pl.ds(rows, HR)], peer(-1, d)),
                   (src.at[hi], dst.at[pl.ds(rows + HR, HR)], peer(1, d)),
                   (src, dst.at[pl.ds(0, rows)], peer(0, d))])
    early = len(waits)
    loaded(2, w_ref)
    send(wrow_n, [(w_ref.at[pl.ds(0, HW)], wrow_n, peer(-1, 0))])
    send(wrow_s, [(w_ref.at[pl.ds(rows - HS, HS)], wrow_s, peer(1, 0))])
    lane8 = lax.broadcasted_iota(jnp.int32, (costs, 128), 1)
    sub8 = lax.broadcasted_iota(jnp.int32, (costs, 128), 0)
    for j in range(rows // 8):
        to_w, to_e = jnp.zeros((costs, 128), jnp.float32), jnp.zeros((costs, 128), jnp.float32)
        for g in range(8):
            at = GROUP * g
            first, last = w_ref[8 * j + g, :, :128], w_ref[8 * j + g, :, cols - 128:]
            to_w = jnp.where((lane8 >= at) & (lane8 < at + HW), roll(first, at, 1), to_w)
            end = at if g else 128
            to_e = jnp.where((lane8 >= end - HS) & (lane8 < end), roll(last, at, 1), to_e)
        wsend_w[j], wsend_e[j] = to_w, to_e
    strips = rows // 8
    for src, dst, d in ((wsend_w, wrecv_e, -1), (wsend_e, wrecv_w, 1)):
        send(dst, [(src, dst.at[pl.ds(0, strips)], peer(0, d)),
                   (src.at[pl.ds(0, 1)], dst.at[pl.ds(strips, 1)], peer(-1, d)),
                   (src.at[pl.ds(strips - 1, 1)], dst.at[pl.ds(strips + 1, 1)], peer(1, d))])
    for c in waits[:early]:
        c.wait_recv()

    full = rows + 2 * HR
    lane = lax.broadcasted_iota(jnp.int32, (full, 128), 1)
    got_e, got_w = recv_e[...], recv_w[...]

    def side(pos, width):
        a = roll(got_e, -pos, 1)
        b = roll(got_w, 128 - width - pos, 1)
        return jnp.where(lane < width, a, jnp.where(lane >= 128 - width, b, 0.0))

    def padded(i):
        if i < 4:
            top, mid, low = row_n[i], wide[i][...], row_s[i]
        else:
            top, mid, low = (r[...].astype(jnp.float32) for r in (mrow_n, mk_ref, mrow_s))
        return jnp.concatenate([jnp.concatenate([mid, top, low], axis=0), side(HC * i, HC)], axis=1)

    ringc = cols + 128
    row_id = lax.broadcasted_iota(jnp.int32, (full, ringc), 0)
    keep_n = (lat < nlat - 1).astype(jnp.float32)
    keep_s = (lat > 0).astype(jnp.float32)
    edge = jnp.where(row_id < rows, 1.0, jnp.where(row_id < rows + HR, keep_n, keep_s))
    wet = padded(4) * edge
    ex = padded(1) * wet * east(wet)
    ey = padded(2) * wet * north(wet)
    base = wet * padded(3) + 1.0 - wet
    diag = base + ex + roll(ex, 1, 1) + ey + roll(ey, 1, 0)
    rs = lax.rsqrt(diag)
    rs = rs * (1.5 - 0.5 * diag * rs * rs)
    rs_e, rs_n = rs * east(rs), rs * north(rs)
    e2 = 2.0 * ex * rs_e
    n2 = 2.0 * ey * rs_n
    e2r[...], n2r[...], rsr[...] = e2, n2, rs
    rz = rows + HB

    lane_r = lax.broadcasted_iota(jnp.int32, (rows, 128), 1)
    row_r = lax.broadcasted_iota(jnp.int32, (rows, 128), 0)

    def to_lanes(column):
        return jnp.broadcast_to(jnp.sum(jnp.where(lane_r == row_r, column, 0.0), axis=0, keepdims=True), (costs, 128))

    def keep(k, u):
        un[k] = u[:rz, :cols]
        us_side[k] = to_lanes(u[:rows, cols:cols + 1])

    def step(k, x, prev, prev2, le, ln, e2, n2):
        s = e2 * le + roll(e2 * prev, 1, 1) + n2 * ln + roll(n2 * prev, 1, 0)
        return s if k == 1 else s - (prev2 + prev2 if k == 2 else prev2)

    us = [rs * padded(0)]
    for k in range(1, ITERS + 1):
        le, ln = east(us[k - 1]), north(us[k - 1])
        keep(k - 1, us[k - 1])
        ue[k - 1], unn[k - 1] = le[:rows, :cols], ln[:rows, :cols]
        us.append(step(k, None, us[k - 1], us[k - 2] if k > 1 else None, le, ln, e2, n2))
    keep(ITERS, us[ITERS])
    up[(ITERS - 1) % 2], up[ITERS % 2] = us[ITERS - 1], us[ITERS]

    inner = [u[:rows, :cols] for u in us]
    rs_in = rs[:rows, :cols]

    mom = ITERS * costs

    def fold(field):
        return total_of(field[i:i + 8, j:j + 128] for i in range(0, rows, 8) for j in range(0, cols, 128))

    mine = jnp.zeros((costs, 128), jnp.float32)
    for k in range(ITERS):
        for m, field in ((2 * k, inner[k] * inner[k]), (2 * k + 1, inner[k] * inner[k + 1])):
            mine = jnp.where(lane8 == mom + m, jnp.sum(fold(field), axis=1, keepdims=True), mine)
    proj = [None] * ITERS
    for r in range(rows):
        wr = w_ref[r] * rsr[r:r + 1, :cols]
        for k in range(ITERS):
            pr = wr * un[k, r:r + 1, :]
            proj[k] = pr if proj[k] is None else proj[k] + pr
    for k in range(ITERS):
        line = total_of(proj[k][:, j:j + 128] for j in range(0, cols, 128))
        mine = jnp.where(lane8 == costs * k + sub8, jnp.sum(line, axis=1, keepdims=True), mine)
    mine = jnp.sum(mine, axis=0, keepdims=True)

    def start(stage, value):
        mailbox, got, ss, rv = reduce_refs[4 * stage:4 * stage + 4]
        mailbox[...] = value
        for i, (a, b) in enumerate(stages[stage]):
            pltpu.make_async_remote_copy(src_ref=mailbox, dst_ref=got.at[i], send_sem=ss, recv_sem=rv,
                                         device_id=peer(a, b), device_id_type=MESH).start()
        all_of = pltpu.make_async_remote_copy(src_ref=got, dst_ref=got, send_sem=ss, recv_sem=rv,
                                              device_id=peer(0, 1), device_id_type=MESH)
        waits.append(all_of)
        return all_of

    def finish(stage, group, value):
        group.wait_recv()
        got = reduce_refs[4 * stage + 1]
        parts = [value] + [got[i] for i in range(len(stages[stage]))]
        while len(parts) > 1:
            parts = [sum(parts[i:i + 2][1:], parts[i]) for i in range(0, len(parts), 2)]
        return parts[0]

    first_reduce = len(waits)
    group = start(0, mine)

    for k in range(ITERS + 1, DEG):
        prev, prev2 = up[(k - 1) % 2], up[k % 2]
        le, ln = east(prev), north(prev)
        ue[k - 1], unn[k - 1] = le[:rows, :cols], ln[:rows, :cols]
        x = step(k, None, prev, prev2, le, ln, e2r[...], n2r[...])
        keep(k, x)
        up[k % 2] = x

    wet_in = wet[:rows, :cols]
    me = wet_in * east(wet)[:rows, :cols]
    mn = wet_in * north(wet)[:rows, :cols]
    geo[0], geo[1] = me, mn
    geo[2] = me * rs_e[:rows, :cols]
    geo[3] = mn * rs_n[:rows, :cols]
    geo[4] = rs_in
    rs_z = rsr[:rz, :cols]
    dia[...] = -0.5 * rs_z * rs_z
    rs_c = rsr[:rows, cols:cols + 1]
    us_side[DEG] = to_lanes(-0.5 * rs_c * rs_c)

    def products(t, carry):
        at = pl.ds(pl.multiple_of(t * 8, 8), 8)
        u = [un[k, at, :] for k in range(DEG)]
        for s in range(DEG):
            acc = None
            for a in range((s + 1) // 2):
                pr = u[a] * u[s - a]
                acc = pr if acc is None else acc + pr
            acc = acc + acc if acc is not None else None
            if s % 2 == 0:
                sq = u[s // 2] * u[s // 2]
                acc = sq if acc is None else acc + sq
            ww[s, at, :] = acc
        return carry

    def cross(t, carry):
        at = pl.ds(pl.multiple_of(t * 8, 8), 8)
        for src, dst in ((ue, xe), (unn, xn)):
            for s in range(DEG - 1):
                acc = None
                for a in range(s + 1):
                    pr = un[a, at, :cols] * src[s - a, at, :]
                    acc = pr if acc is None else acc + pr
                dst[s, at, :] = acc
        return carry

    lax.fori_loop(0, rz // 8, products, 0)
    lax.fori_loop(0, rows // 8, cross, 0)

    for c in waits[early:first_reduce]:
        c.wait_recv()

    for j in range(strips + 2):
        comb[j] = jnp.where(lane8 % GROUP < HW, wrecv_e[j], wrecv_w[j])

    def ring_row(r):
        return r if r >= 0 else full + r

    def line(ref, r):
        q = ring_row(r)
        return ref[q:q + 1, :]

    for r in range(-HS, rows + HW):
        if r < 0:
            block, packed, g = wrow_s[r + HS], comb[strips + 1], 8 + r
        elif r >= rows:
            block, packed, g = wrow_n[r - rows], comb[strips], r - rows
        else:
            block, packed, g = w_ref[r], comb[r // 8], r % 8
        side_r = roll(packed, -GROUP * g, 1)
        v[0, r + HS] = line(rsr, r) * jnp.concatenate([block, side_r], axis=1)

    for k in range(1, ITERS):
        for r in range(k - HS, rows + HW - k):
            x = v[k - 1, r + HS]
            e = line(e2r, r)
            le = east(x)
            y = e * le + roll(e * x, 1, 1) + line(n2r, r) * v[k - 1, r + HS + 1] + line(n2r, r - 1) * v[k - 1, r + HS - 1]
            if k > 1:
                before = v[k - 2, r + HS]
                y = y - (before + before if k == 2 else before)
            v[k, r + HS] = y
            if 0 <= r < rows:
                ve[k - 1, r] = le[:, :cols]
    for k in range(ITERS):
        acc = jnp.zeros((costs, 128), jnp.float32)
        for r in range(rows):
            acc = jnp.where(lane8 == r, roll(v[k, r + HS, :, cols:], r, 1), acc)
        vs_side[k] = acc

    total = finish(0, group, mine)
    for stage in range(1, len(stages)):
        total = finish(stage, start(stage, total), total)

    tot8 = jnp.broadcast_to(total, (costs, 128))
    def pick(index):
        return jnp.broadcast_to(
            jnp.sum(jnp.where(lane8 == index, tot8, 0.0), axis=1, keepdims=True), (costs, 128))

    proj = [pick(k * costs + sub8) * (0.5 if k else 1.0) for k in range(ITERS)]
    raw = [pick(mom + m) * (0.5 if m == 1 else 0.25 if m else 1.0) for m in range(DEG)]
    mu = [raw[0], raw[1]]
    for k in range(1, ITERS):
        mu += [2.0 * raw[2 * k] - raw[0], 2.0 * raw[2 * k + 1] - raw[1]]
    c, bar = coefficients(mu, proj)
    zero = jnp.zeros_like(c[0])
    acc = [zero] * (ITERS + 2)
    for m in range(ITERS - 1, -1, -1):
        acc[m] = c[m] + acc[m + 2]
    tail = [zero] * (DEG + 2)
    for m in range(DEG - 1, -1, -1):
        tail[m] = bar[m] + tail[m + 2]
    for m in range(ITERS):
        coef[CS + m] = acc[m]
        coef[CC + m] = 0.5 * c[m] if m else c[m]
    for s in range(DEG - 1):
        coef[CX + s] = 2.0 * tail[s + 1]
    for s in range(DEG):
        coef[CH + s] = tail[s] + tail[s + 2] if s else 2.0 * tail[0]
        coef[CM + s] = bar[s] if s else 2.0 * bar[0]
    for c in waits:
        c.wait_send()


def adjoint_kernel(un, ue, xe, xn, ww, v, ve, geo, dia, coef, us_side, vs_side,
                   fa_hbm, ge_hbm, gn_hbm, y, ye, z, fa_ref, ge_ref, gn_ref, osem):
    rows, costs, cols = fa_ref.shape
    rz = dia.shape[0]

    outs = ((fa_ref, fa_hbm), (ge_ref, ge_hbm), (gn_ref, gn_hbm))

    def factor(i, width, at=None):
        c = coef[i] if at is None else coef[i, at:at + 1]
        return jnp.concatenate([c] * (width // 128), axis=1)

    def vectors(u, width, at):
        return [total_of(factor(CS + a + b + 1, width, at) * u[b] for b in range(ITERS - 1 - a))
                for a in range(-1, ITERS - 1)]

    def diagonal(ys, u, width, at):
        out = [ys[0] + ys[2] + factor(CC, width, at) * u[0]]
        return out + [ys[a] + ys[a + 2] if a + 2 < len(ys) else ys[a] for a in range(1, ITERS)]

    def combine(t, carry):
        at = pl.ds(pl.multiple_of(t * 8, 8), 8)
        u = [un[k, at, :] for k in range(ITERS)]
        ys = vectors(u, cols, 0)
        for a, f in enumerate(diagonal(ys, u, cols, 0)):
            z[a, at, :] = f
        for a in range(ITERS - 1):
            y[a, at, :] = ys[a + 1]
        return carry

    def combine_east(t, carry):
        at = pl.ds(pl.multiple_of(t * 8, 8), 8)
        u = [ue[k, at, :] for k in range(ITERS - 1)]
        for a in range(ITERS - 1):
            ye[a, at, :] = total_of(factor(CS + a + b + 1, cols, 0) * u[b] for b in range(ITERS - 1 - a))
        return carry

    lax.fori_loop(0, rz // 8, combine, 0)
    lax.fori_loop(0, rows // 8, combine_east, 0)
    u = [us_side[k] for k in range(DEG)]
    zs = diagonal(vectors(u, 128, None), u, 128, None)
    side = total_of(zs[a] * vs_side[a] for a in range(ITERS))
    for s in range(DEG):
        side = side + coef[CH + s] * total_of(u[a] * u[s - a] for a in range(s + 1))
    side = side * us_side[DEG]
    lane_c = lax.broadcasted_iota(jnp.int32, (costs, cols), 1)

    def line(ref, *at):
        return ref[(*at[:-1], pl.ds(at[-1], 1), slice(None))]

    def diag_of(r):
        acc = total_of(line(z, a, r) * v[a, r + HS, :, :cols] for a in range(ITERS))
        for s in range(DEG):
            acc = acc + factor(CH + s, cols) * line(ww, s, r)
        return acc * line(dia, r)

    def row(r, above):
        ge = gn = fa = db = None

        def add(acc, term):
            return term if acc is None else acc + term

        for a in range(ITERS):
            x = v[a, r + HS, :, :cols]
            db = add(db, x * line(z, a, r))
            fa = add(fa, x * factor(CC + a, cols))
            if a < ITERS - 1:
                here = line(y, a, r)
                ge = add(ge, x * line(ye, a, r) + ve[a, r] * here)
                gn = add(gn, x * line(y, a, r + 1) + v[a, r + HS + 1, :, :cols] * here)
        for s in range(DEG):
            db = add(db, factor(CH + s, cols) * line(ww, s, r))
            fa = add(fa, factor(CM + s, cols) * line(un, s, r))
            if s < DEG - 1:
                c = factor(CX + s, cols)
                ge = add(ge, c * line(xe, s, r))
                gn = add(gn, c * line(xn, s, r))
        db = db * line(dia, r)
        end = jnp.concatenate([pltpu.roll(side, 127 - r, 1)] * (cols // 128), axis=1)
        db_e = jnp.where(lane_c == cols - 1, end, east(db))
        fa_ref[r] = line(geo, 4, r) * fa
        ge_ref[r] = line(geo, 2, r) * ge + line(geo, 0, r) * (db + db_e)
        gn_ref[r] = line(geo, 3, r) * gn + line(geo, 1, r) * (db + above)
        return db

    parts = 2
    size = rows // parts

    def block(i, above):
        first = rows - (i + 1) * BLOCK
        for j in range(BLOCK - 1, -1, -1):
            above = row(first + j, above)
        return above

    above = diag_of(rows)
    per = size // BLOCK
    for p in range(parts):
        above = lax.fori_loop(p * per, (p + 1) * per, block, above)
        at = pl.ds(rows - (p + 1) * size, size)
        for i, (src, dst) in enumerate(outs):
            for n in range(costs):
                pltpu.make_async_copy(src.at[at, n, :], dst.at[n, at], osem.at[i]).start()
    for i, (src, dst) in enumerate(outs):
        pltpu.make_async_copy(dst, dst, osem.at[i]).wait()


def solution(mesh):
    nlat, nlon = mesh.shape["lat"], mesh.shape["lon"]

    def body(forcing, depth_east, depth_north, surface_term, ocean_mask, cost_weights):
        costs, rows, cols = cost_weights.shape
        full, ringc = rows + 2 * HR, cols + 128
        f32 = jnp.float32
        dma = pltpu.SemaphoreType.DMA
        every = [(a, b) for a in range(nlat) for b in range(nlon) if a or b]
        stages = [every] if len(every) < 64 else [
            [(0, b) for b in range(1, nlon)], [(a, 0) for a in range(1, nlat)]]
        reduce_scratch = [
            ref for g in stages for ref in (
                pltpu.VMEM((1, 128), f32), pltpu.VMEM((len(g), 1, 128), f32),
                dma, dma)]
        rz = rows + HB
        shapes = (
            (DEG, rz, cols), (DEG - 1, rows, cols), (DEG - 1, rows, cols), (DEG - 1, rows, cols), (DEG, rz, cols),
            (ITERS, rows + HS + HW, costs, ringc), (ITERS - 1, rows, costs, cols),
            (5, rows, cols), (rz, cols), (NCOEF, costs, 128), (DEG + 1, costs, 128), (ITERS, costs, 128))
        hbm = pl.BlockSpec(memory_space=pltpu.HBM)
        vmem = pl.BlockSpec(memory_space=pltpu.VMEM)
        args = (forcing, depth_east, depth_north, surface_term, ocean_mask, cost_weights)
        mids = pl.pallas_call(
            functools.partial(kernel, nlat, nlon, stages),
            out_shape=[pltpu.VMEM(x, f32) for x in shapes],
            in_specs=[hbm] * 6,
            out_specs=[vmem] * len(shapes),
            scratch_shapes=[
                pltpu.VMEM((4, rows, cols), f32),
                pltpu.VMEM((rows, cols), jnp.int32),
                pltpu.VMEM((rows, costs, cols), f32),
                dma((3,)),
                pltpu.VMEM((rows, 128), f32),
                pltpu.VMEM((rows, 128), f32),
                pltpu.VMEM((full, 128), f32),
                pltpu.VMEM((full, 128), f32),
                pltpu.VMEM((4, HR, cols), f32),
                pltpu.VMEM((4, HR, cols), f32),
                pltpu.VMEM((HR, cols), jnp.int32),
                pltpu.VMEM((HR, cols), jnp.int32),
                pltpu.VMEM((HW, costs, cols), f32),
                pltpu.VMEM((HS, costs, cols), f32),
                *[pltpu.VMEM((rows // 8, costs, 128), f32)] * 2,
                *[pltpu.VMEM((rows // 8 + 2, costs, 128), f32)] * 2,
                pltpu.VMEM((2, full, ringc), f32),
                pltpu.VMEM((DEG - 1, rows, cols), f32),
                *[pltpu.VMEM((full, ringc), f32)] * 3,
                pltpu.VMEM((rows // 8 + 2, costs, 128), f32),
                dma((10,)),
                dma((10,)),
                *reduce_scratch,
            ],
            compiler_params=pltpu.CompilerParams(
                collective_id=0, has_side_effects=True, vmem_limit_bytes=24 * 1024 * 1024
            ),
        )(*[pltpu.with_memory_space_constraint(x, pltpu.HBM) for x in args])
        out = (costs, rows, cols)
        return pl.pallas_call(
            adjoint_kernel,
            out_shape=[jax.ShapeDtypeStruct(out, f32)] * 3,
            in_specs=[vmem] * len(shapes),
            out_specs=[hbm] * 3,
            scratch_shapes=[
                pltpu.VMEM((ITERS - 1, rz, cols), f32),
                pltpu.VMEM((ITERS - 1, rows, cols), f32),
                pltpu.VMEM((ITERS, rz, cols), f32),
                *[pltpu.VMEM((rows, costs, cols), f32)] * 3,
                dma((3,)),
            ],
            compiler_params=pltpu.CompilerParams(vmem_limit_bytes=24 * 1024 * 1024),
        )(*[pltpu.with_memory_space_constraint(x, pltpu.VMEM) for x in mids])

    grid = P("lat", "lon")
    field = P(None, "lat", "lon")
    return jax.shard_map(
        body,
        mesh=mesh,
        in_specs=(grid, grid, grid, grid, grid, field),
        out_specs=(field, field, field),
        check_vma=False,
    )
```

```python
import functools

import jax
import jax.numpy as jnp
from jax import lax
from jax.experimental import pallas as pl
from jax.experimental.pallas import tpu as pltpu
from jax.sharding import PartitionSpec as P

ITERS = 6
MESH = pl.DeviceIdType.MESH
HB = 8
HS = 5
BLOCK = 8
HC = 13
HW = 6
GROUP = 16
DEG = 2 * ITERS
CS, CC = 0, ITERS
CX = CC + ITERS
CH = CX + DEG - 1
CM = CH + DEG
NCOEF = CM + DEG


def coefficients(mu, proj):
    def gram(a, b):
        return 0.5 * (mu[a + b] + mu[abs(a - b)])

    h = {}
    for a in range(ITERS):
        for b in range(a, ITERS):
            h[a, b] = gram(a, b) - 0.5 * (gram(a, b + 1) + gram(a, abs(b - 1)))
    g, p = list(mu[:ITERS]), list(proj)
    low, inv = {}, []
    for i in range(ITERS):
        inv.append(1.0 / h[i, i])
        for j in range(i + 1, ITERS):
            low[j, i] = h[i, j] * inv[i]
        for j in range(i + 1, ITERS):
            for k in range(j, ITERS):
                h[j, k] = h[j, k] - low[j, i] * h[i, k]
            g[j] = g[j] - low[j, i] * g[i]
            p[j] = p[j] - low[j, i] * p[i]
    c, d = [None] * ITERS, [None] * ITERS
    for i in range(ITERS - 1, -1, -1):
        c[i], d[i] = g[i] * inv[i], p[i] * inv[i]
        for j in range(i + 1, ITERS):
            c[i] = c[i] - low[j, i] * c[j]
            d[i] = d[i] - low[j, i] * d[j]
    zero = jnp.zeros_like(c[0])
    cc = c + [zero, zero]
    res = [1.0 - c[0] + 0.5 * c[1], c[0] + 0.5 * cc[2] - c[1]]
    for j in range(2, ITERS + 1):
        res.append(0.5 * (cc[j - 1] + cc[j + 1]) - cc[j])
    bar = [zero] * DEG
    for a in range(ITERS):
        half = 0.5 * d[a]
        for j in range(ITERS + 1):
            t = half * res[j]
            bar[a + j] = bar[a + j] + t
            bar[abs(a - j)] = bar[abs(a - j)] + t
    return c, bar


def roll(x, shift, axis):
    return pltpu.roll(x, shift % x.shape[axis], axis)


def east(x):
    return roll(x, -1, 1)


def north(x):
    return roll(x, -1, 0)


def total_of(terms):
    acc = None
    for t in terms:
        acc = t if acc is None else acc + t
    return acc


def kernel(nlat, nlon, stages, f_hbm, de_hbm, dn_hbm, st_hbm, mk_hbm, w_hbm,
           un, ue, xe, xn, ww, v, ve, geo, dia, coef, us_side, vs_side,
           fields, mk_ref, w_ref, lsem,
           send_w, send_e, recv_e, recv_w, far_e, far_w, row_n, row_s, far_n, far_s,
           mrow_n, mrow_s, mfar_n, mfar_s, wrow_n, wrow_s,
           wsend_w, wsend_e, wrecv_e, wrecv_w, up, unn, e2r, n2r, rsr, e2w, n2w, comb, ssem, rsem, hello,
           *reduce_refs):
    lat, lon = lax.axis_index("lat"), lax.axis_index("lon")
    rows, costs, cols = w_ref.shape
    for i, src in enumerate((f_hbm, de_hbm, dn_hbm, st_hbm)):
        pltpu.make_async_copy(src, fields.at[i], lsem.at[0]).start()
    pltpu.make_async_copy(mk_hbm, mk_ref, lsem.at[1]).start()
    for n in range(costs):
        pltpu.make_async_copy(w_hbm.at[n], w_ref.at[:, n, :], lsem.at[2]).start()

    def loaded(i, ref):
        pltpu.make_async_copy(ref, ref, lsem.at[i]).wait()

    def peer(dlat, dlon):
        return (lax.rem(lat + dlat + nlat, nlat), lax.rem(lon + dlon + nlon, nlon))

    def ring(radius, lat_too, lon_too):
        offs = {(a % nlat, b % nlon) for a in ((-radius, 0, radius) if lat_too else (0,))
                for b in ((-radius, 0, radius) if lon_too else (0,))}
        return sorted(offs - {(0, 0)})

    def greet(sem, offs):
        for a, b in offs:
            pl.semaphore_signal(sem, inc=1, device_id=peer(a, b), device_id_type=MESH)

    barrier = pltpu.get_barrier_semaphore()
    near = ring(1, True, True)
    rounds, radius = [], 1
    while radius < max(nlat // 2, nlon // 2):
        rounds.append(ring(radius, radius < nlat // 2, radius < nlon // 2))
        radius *= 2
    greet(barrier, near)

    loaded(0, fields)
    loaded(1, mk_ref)

    lane = lax.broadcasted_iota(jnp.int32, (rows, 128), 1)
    wide = [fields.at[i] for i in range(4)] + [mk_ref]
    for ref, at, first in ((send_w, slice(0, 128), True), (send_e, slice(cols - 128, cols), False)):
        buf = jnp.zeros((rows, 128), jnp.float32)
        for i in range(5):
            pos = HC * i
            tile = wide[i][:, at].astype(jnp.float32)
            tile = roll(tile, pos if first else pos + HC, 1)
            buf = jnp.where((lane >= pos) & (lane < pos + HC), tile, buf)
        ref[...] = buf
    pl.semaphore_wait(barrier, len(near))
    if rounds:
        greet(hello.at[0], rounds[0])

    waits = []

    def send(whole, parts):
        i = len(waits)
        for src, dst, dev in parts:
            pltpu.make_async_remote_copy(src_ref=src, dst_ref=dst, send_sem=ssem.at[i], recv_sem=rsem.at[i],
                                         device_id=dev, device_id_type=MESH).start()
        waits.append(pltpu.make_async_remote_copy(src_ref=whole, dst_ref=whole, send_sem=ssem.at[i],
                                                  recv_sem=rsem.at[i], device_id=peer(0, 1), device_id_type=MESH))

    lo, hi, lo2, hi2 = (pl.ds(i, HB) for i in (0, rows - HB, HB, rows - 2 * HB))
    send(row_n, [(fields.at[:, lo], row_n, peer(-1, 0))])
    send(row_s, [(fields.at[:, hi], row_s, peer(1, 0))])
    send(mrow_n, [(mk_ref.at[lo], mrow_n, peer(-1, 0))])
    send(mrow_s, [(mk_ref.at[hi], mrow_s, peer(1, 0))])
    sides = ((send_w, recv_e, far_e, -1), (send_e, recv_w, far_w, 1))
    for src, dst, far, d in sides:
        send(dst, [(src.at[lo], dst.at[pl.ds(rows, HB)], peer(-1, d)),
                   (src.at[hi], dst.at[pl.ds(rows + HB, HB)], peer(1, d)),
                   (src, dst.at[pl.ds(0, rows)], peer(0, d))])
    early = len(waits)
    send(far_n, [(fields.at[:, lo2], far_n, peer(-1, 0))])
    send(far_s, [(fields.at[:, hi2], far_s, peer(1, 0))])
    send(mfar_n, [(mk_ref.at[lo2], mfar_n, peer(-1, 0))])
    send(mfar_s, [(mk_ref.at[hi2], mfar_s, peer(1, 0))])
    for src, dst, far, d in sides:
        send(far, [(src.at[lo2], far.at[pl.ds(0, HB)], peer(-1, d)),
                   (src.at[hi2], far.at[pl.ds(HB, HB)], peer(1, d))])
    late = len(waits)
    loaded(2, w_ref)
    send(wrow_n, [(w_ref.at[pl.ds(0, HW)], wrow_n, peer(-1, 0))])
    send(wrow_s, [(w_ref.at[pl.ds(rows - HS, HS)], wrow_s, peer(1, 0))])
    lane8 = lax.broadcasted_iota(jnp.int32, (costs, 128), 1)
    sub8 = lax.broadcasted_iota(jnp.int32, (costs, 128), 0)
    for j in range(rows // 8):
        to_w, to_e = jnp.zeros((costs, 128), jnp.float32), jnp.zeros((costs, 128), jnp.float32)
        for g in range(8):
            at = GROUP * g
            first, last = w_ref[8 * j + g, :, :128], w_ref[8 * j + g, :, cols - 128:]
            to_w = jnp.where((lane8 >= at) & (lane8 < at + HW), roll(first, at, 1), to_w)
            end = at if g else 128
            to_e = jnp.where((lane8 >= end - HS) & (lane8 < end), roll(last, at, 1), to_e)
        wsend_w[j], wsend_e[j] = to_w, to_e
    strips = rows // 8
    for src, dst, d in ((wsend_w, wrecv_e, -1), (wsend_e, wrecv_w, 1)):
        send(dst, [(src, dst.at[pl.ds(0, strips)], peer(0, d)),
                   (src.at[pl.ds(0, 1)], dst.at[pl.ds(strips, 1)], peer(-1, d)),
                   (src.at[pl.ds(strips - 1, 1)], dst.at[pl.ds(strips + 1, 1)], peer(1, d))])
    for i in range(1, len(rounds)):
        pl.semaphore_wait(hello.at[i - 1], len(rounds[i - 1]))
        greet(hello.at[i], rounds[i])
    for c in waits[:early]:
        c.wait_recv()

    full = rows + 2 * HB
    keep_n = (lat < nlat - 1).astype(jnp.float32)
    keep_s = (lat > 0).astype(jnp.float32)

    def operator(mains, got_e, got_w, runs):
        height = got_e.shape[0]
        lane = lax.broadcasted_iota(jnp.int32, (height, 128), 1)

        def padded(i):
            a = roll(got_e, -HC * i, 1)
            b = roll(got_w, 128 - HC - HC * i, 1)
            side = jnp.where(lane < HC, a, jnp.where(lane >= 128 - HC, b, 0.0))
            return jnp.concatenate([mains(i), side], axis=1)

        edge = jnp.concatenate([jnp.full((n, cols + 128), k, jnp.float32) for n, k in runs], axis=0)
        wet = padded(4) * edge
        ex = padded(1) * wet * east(wet)
        ey = padded(2) * wet * north(wet)
        base = wet * padded(3) + 1.0 - wet
        diag = base + ex + roll(ex, 1, 1) + ey + roll(ey, 1, 0)
        rs = lax.rsqrt(diag)
        rs = rs * (1.5 - 0.5 * diag * rs * rs)
        rs_e, rs_n = rs * east(rs), rs * north(rs)
        return wet, rs, rs_e, rs_n, 2.0 * ex * rs_e, 2.0 * ey * rs_n, rs * padded(0)

    def stacked(order):
        def mains(i):
            if i < 4:
                return jnp.concatenate([ref[i] if at is None else ref[i, at] for ref, _, at in order], axis=0)
            return jnp.concatenate([(ref[...] if at is None else ref[at]) for _, ref, at in order],
                                   axis=0).astype(jnp.float32)
        return mains

    wet, rs, rs_e, rs_n, e2, n2, u0 = operator(
        stacked(((fields, mk_ref, None), (row_n, mrow_n, None), (row_s, mrow_s, None))),
        recv_e[...], recv_w[...], ((rows, 1.0), (HB, keep_n), (HB, keep_s)))
    e2r[...], n2r[...], rsr[...] = e2, n2, rs
    rz = rows + HB

    lane_r = lax.broadcasted_iota(jnp.int32, (rows, 128), 1)
    row_r = lax.broadcasted_iota(jnp.int32, (rows, 128), 0)

    def to_lanes(column):
        return jnp.broadcast_to(jnp.sum(jnp.where(lane_r == row_r, column, 0.0), axis=0, keepdims=True), (costs, 128))

    def keep(k, u):
        un[k] = u[:rz, :cols]
        us_side[k] = to_lanes(u[:rows, cols:cols + 1])

    def step(k, x, prev, prev2, le, ln, e2, n2):
        s = e2 * le + roll(e2 * prev, 1, 1) + n2 * ln + roll(n2 * prev, 1, 0)
        return s if k == 1 else s - (prev2 + prev2 if k == 2 else prev2)

    us = [u0]
    for k in range(1, ITERS + 1):
        le, ln = east(us[k - 1]), north(us[k - 1])
        keep(k - 1, us[k - 1])
        ue[k - 1], unn[k - 1] = le[:rows, :cols], ln[:rows, :cols]
        us.append(step(k, None, us[k - 1], us[k - 2] if k > 1 else None, le, ln, e2, n2))
    keep(ITERS, us[ITERS])

    inner = [u[:rows, :cols] for u in us]
    rs_in = rs[:rows, :cols]

    mom = ITERS * costs

    def fold(field):
        return total_of(field[i:i + 8, j:j + 128] for i in range(0, rows, 8) for j in range(0, cols, 128))

    mine = jnp.zeros((costs, 128), jnp.float32)
    for k in range(ITERS):
        for m, field in ((2 * k, inner[k] * inner[k]), (2 * k + 1, inner[k] * inner[k + 1])):
            mine = jnp.where(lane8 == mom + m, jnp.sum(fold(field), axis=1, keepdims=True), mine)
    proj = [None] * ITERS
    for r in range(rows):
        wr = w_ref[r] * rsr[r:r + 1, :cols]
        for k in range(ITERS):
            pr = wr * un[k, r:r + 1, :]
            proj[k] = pr if proj[k] is None else proj[k] + pr
    for k in range(ITERS):
        line = total_of(proj[k][:, j:j + 128] for j in range(0, cols, 128))
        mine = jnp.where(lane8 == costs * k + sub8, jnp.sum(line, axis=1, keepdims=True), mine)
    mine = jnp.sum(mine, axis=0, keepdims=True)

    def start(stage, value):
        mailbox, got, ss, rv = reduce_refs[4 * stage:4 * stage + 4]
        mailbox[...] = value
        for i, (a, b) in enumerate(stages[stage]):
            pltpu.make_async_remote_copy(src_ref=mailbox, dst_ref=got.at[i], send_sem=ss, recv_sem=rv,
                                         device_id=peer(a, b), device_id_type=MESH).start()
        all_of = pltpu.make_async_remote_copy(src_ref=got, dst_ref=got, send_sem=ss, recv_sem=rv,
                                              device_id=peer(0, 1), device_id_type=MESH)
        waits.append(all_of)
        return all_of

    def finish(stage, group, value):
        group.wait_recv()
        got = reduce_refs[4 * stage + 1]
        parts = [value] + [got[i] for i in range(len(stages[stage]))]
        while len(parts) > 1:
            parts = [sum(parts[i:i + 2][1:], parts[i]) for i in range(0, len(parts), 2)]
        return parts[0]

    first_reduce = len(waits)
    if rounds:
        pl.semaphore_wait(hello.at[len(rounds) - 1], len(rounds[-1]))
    group = start(0, mine)

    for c in waits[early:late]:
        c.wait_recv()

    def band_of(near, far):
        return jnp.concatenate([near[rows - HB:rows], near[rows:rows + HB], far[...],
                                near[rows + HB:], near[:HB]], axis=0)

    low, high = slice(rows - HB, rows), slice(0, HB)
    _, _, _, _, e2b, n2b, b0 = operator(
        stacked(((fields, mk_ref, low), (row_n, mrow_n, None), (far_n, mfar_n, None),
                 (far_s, mfar_s, None), (row_s, mrow_s, None), (fields, mk_ref, high))),
        band_of(recv_e, far_e), band_of(recv_w, far_w),
        ((HB, 1.0), (2 * HB, keep_n), (2 * HB, keep_s), (HB, 1.0)))
    band = [b0]
    for k in range(1, ITERS + 1):
        band.append(step(k, None, band[-1], band[-2] if k > 1 else None, east(band[-1]), north(band[-1]), e2b, n2b))

    def joined(main, halo):
        return jnp.concatenate([main[:rows], halo[HB:5 * HB]], axis=0)

    e2w[...], n2w[...] = joined(e2, e2b), joined(n2, n2b)
    for k in (ITERS - 1, ITERS):
        up[k % 2] = joined(us[k], band[k])
    for k in range(ITERS + 1, DEG):
        prev, prev2 = up[(k - 1) % 2], up[k % 2]
        le, ln = east(prev), north(prev)
        ue[k - 1], unn[k - 1] = le[:rows, :cols], ln[:rows, :cols]
        x = step(k, None, prev, prev2, le, ln, e2w[...], n2w[...])
        keep(k, x)
        up[k % 2] = x

    wet_in = wet[:rows, :cols]
    me = wet_in * east(wet)[:rows, :cols]
    mn = wet_in * north(wet)[:rows, :cols]
    geo[0], geo[1] = me, mn
    geo[2] = me * rs_e[:rows, :cols]
    geo[3] = mn * rs_n[:rows, :cols]
    geo[4] = rs_in
    rs_z = rsr[:rz, :cols]
    dia[...] = -0.5 * rs_z * rs_z
    rs_c = rsr[:rows, cols:cols + 1]
    us_side[DEG] = to_lanes(-0.5 * rs_c * rs_c)

    def products(t, carry):
        at = pl.ds(pl.multiple_of(t * 8, 8), 8)
        u = [un[k, at, :] for k in range(DEG)]
        for s in range(DEG):
            acc = None
            for a in range((s + 1) // 2):
                pr = u[a] * u[s - a]
                acc = pr if acc is None else acc + pr
            acc = acc + acc if acc is not None else None
            if s % 2 == 0:
                sq = u[s // 2] * u[s // 2]
                acc = sq if acc is None else acc + sq
            ww[s, at, :] = acc
        return carry

    def cross(t, carry):
        at = pl.ds(pl.multiple_of(t * 8, 8), 8)
        for src, dst in ((ue, xe), (unn, xn)):
            for s in range(DEG - 1):
                acc = None
                for a in range(s + 1):
                    pr = un[a, at, :cols] * src[s - a, at, :]
                    acc = pr if acc is None else acc + pr
                dst[s, at, :] = acc
        return carry

    lax.fori_loop(0, rz // 8, products, 0)
    lax.fori_loop(0, rows // 8, cross, 0)

    for c in waits[late:first_reduce]:
        c.wait_recv()

    for j in range(strips + 2):
        comb[j] = jnp.where(lane8 % GROUP < HW, wrecv_e[j], wrecv_w[j])

    def ring_row(r):
        return r if r >= 0 else full + r

    def line(ref, r):
        q = ring_row(r)
        return ref[q:q + 1, :]

    for r in range(-HS, rows + HW):
        if r < 0:
            block, packed, g = wrow_s[r + HS], comb[strips + 1], 8 + r
        elif r >= rows:
            block, packed, g = wrow_n[r - rows], comb[strips], r - rows
        else:
            block, packed, g = w_ref[r], comb[r // 8], r % 8
        side_r = roll(packed, -GROUP * g, 1)
        v[0, r + HS] = line(rsr, r) * jnp.concatenate([block, side_r], axis=1)

    for k in range(1, ITERS):
        for r in range(k - HS, rows + HW - k):
            x = v[k - 1, r + HS]
            e = line(e2r, r)
            le = east(x)
            y = e * le + roll(e * x, 1, 1) + line(n2r, r) * v[k - 1, r + HS + 1] + line(n2r, r - 1) * v[k - 1, r + HS - 1]
            if k > 1:
                before = v[k - 2, r + HS]
                y = y - (before + before if k == 2 else before)
            v[k, r + HS] = y
            if 0 <= r < rows:
                ve[k - 1, r] = le[:, :cols]
    for k in range(ITERS):
        acc = jnp.zeros((costs, 128), jnp.float32)
        for r in range(rows):
            acc = jnp.where(lane8 == r, roll(v[k, r + HS, :, cols:], r, 1), acc)
        vs_side[k] = acc

    total = finish(0, group, mine)
    for stage in range(1, len(stages)):
        total = finish(stage, start(stage, total), total)

    tot8 = jnp.broadcast_to(total, (costs, 128))
    def pick(index):
        return jnp.broadcast_to(
            jnp.sum(jnp.where(lane8 == index, tot8, 0.0), axis=1, keepdims=True), (costs, 128))

    proj = [pick(k * costs + sub8) * (0.5 if k else 1.0) for k in range(ITERS)]
    raw = [pick(mom + m) * (0.5 if m == 1 else 0.25 if m else 1.0) for m in range(DEG)]
    mu = [raw[0], raw[1]]
    for k in range(1, ITERS):
        mu += [2.0 * raw[2 * k] - raw[0], 2.0 * raw[2 * k + 1] - raw[1]]
    c, bar = coefficients(mu, proj)
    zero = jnp.zeros_like(c[0])
    acc = [zero] * (ITERS + 2)
    for m in range(ITERS - 1, -1, -1):
        acc[m] = c[m] + acc[m + 2]
    tail = [zero] * (DEG + 2)
    for m in range(DEG - 1, -1, -1):
        tail[m] = bar[m] + tail[m + 2]
    for m in range(ITERS):
        coef[CS + m] = acc[m]
        coef[CC + m] = 0.5 * c[m] if m else c[m]
    for s in range(DEG - 1):
        coef[CX + s] = 2.0 * tail[s + 1]
    for s in range(DEG):
        coef[CH + s] = tail[s] + tail[s + 2] if s else 2.0 * tail[0]
        coef[CM + s] = bar[s] if s else 2.0 * bar[0]
    for c in waits:
        c.wait_send()


def adjoint_kernel(un, ue, xe, xn, ww, v, ve, geo, dia, coef, us_side, vs_side,
                   fa_hbm, ge_hbm, gn_hbm, y, ye, z, fa_ref, ge_ref, gn_ref, osem):
    rows, costs, cols = fa_ref.shape
    rz = dia.shape[0]

    outs = ((fa_ref, fa_hbm), (ge_ref, ge_hbm), (gn_ref, gn_hbm))

    def factor(i, width, at=None):
        c = coef[i] if at is None else coef[i, at:at + 1]
        return jnp.concatenate([c] * (width // 128), axis=1)

    def vectors(u, width, at):
        return [total_of(factor(CS + a + b + 1, width, at) * u[b] for b in range(ITERS - 1 - a))
                for a in range(-1, ITERS - 1)]

    def diagonal(ys, u, width, at):
        out = [ys[0] + ys[2] + factor(CC, width, at) * u[0]]
        return out + [ys[a] + ys[a + 2] if a + 2 < len(ys) else ys[a] for a in range(1, ITERS)]

    def combine(t, carry):
        at = pl.ds(pl.multiple_of(t * 8, 8), 8)
        u = [un[k, at, :] for k in range(ITERS)]
        ys = vectors(u, cols, 0)
        for a, f in enumerate(diagonal(ys, u, cols, 0)):
            z[a, at, :] = f
        for a in range(ITERS - 1):
            y[a, at, :] = ys[a + 1]
        return carry

    def combine_east(t, carry):
        at = pl.ds(pl.multiple_of(t * 8, 8), 8)
        u = [ue[k, at, :] for k in range(ITERS - 1)]
        for a in range(ITERS - 1):
            ye[a, at, :] = total_of(factor(CS + a + b + 1, cols, 0) * u[b] for b in range(ITERS - 1 - a))
        return carry

    lax.fori_loop(0, rz // 8, combine, 0)
    lax.fori_loop(0, rows // 8, combine_east, 0)
    u = [us_side[k] for k in range(DEG)]
    zs = diagonal(vectors(u, 128, None), u, 128, None)
    side = total_of(zs[a] * vs_side[a] for a in range(ITERS))
    for s in range(DEG):
        side = side + coef[CH + s] * total_of(u[a] * u[s - a] for a in range(s + 1))
    side = side * us_side[DEG]
    lane_c = lax.broadcasted_iota(jnp.int32, (costs, cols), 1)

    def line(ref, *at):
        return ref[(*at[:-1], pl.ds(at[-1], 1), slice(None))]

    def diag_of(r):
        acc = total_of(line(z, a, r) * v[a, r + HS, :, :cols] for a in range(ITERS))
        for s in range(DEG):
            acc = acc + factor(CH + s, cols) * line(ww, s, r)
        return acc * line(dia, r)

    def row(r, above):
        ge = gn = fa = db = None

        def add(acc, term):
            return term if acc is None else acc + term

        for a in range(ITERS):
            x = v[a, r + HS, :, :cols]
            db = add(db, x * line(z, a, r))
            fa = add(fa, x * factor(CC + a, cols))
            if a < ITERS - 1:
                here = line(y, a, r)
                ge = add(ge, x * line(ye, a, r) + ve[a, r] * here)
                gn = add(gn, x * line(y, a, r + 1) + v[a, r + HS + 1, :, :cols] * here)
        for s in range(DEG):
            db = add(db, factor(CH + s, cols) * line(ww, s, r))
            fa = add(fa, factor(CM + s, cols) * line(un, s, r))
            if s < DEG - 1:
                c = factor(CX + s, cols)
                ge = add(ge, c * line(xe, s, r))
                gn = add(gn, c * line(xn, s, r))
        db = db * line(dia, r)
        end = jnp.concatenate([pltpu.roll(side, 127 - r, 1)] * (cols // 128), axis=1)
        db_e = jnp.where(lane_c == cols - 1, end, east(db))
        fa_ref[r] = line(geo, 4, r) * fa
        ge_ref[r] = line(geo, 2, r) * ge + line(geo, 0, r) * (db + db_e)
        gn_ref[r] = line(geo, 3, r) * gn + line(geo, 1, r) * (db + above)
        return db

    parts = 2
    size = rows // parts

    def block(i, above):
        first = rows - (i + 1) * BLOCK
        for j in range(BLOCK - 1, -1, -1):
            above = row(first + j, above)
        return above

    above = diag_of(rows)
    per = size // BLOCK
    for p in range(parts):
        above = lax.fori_loop(p * per, (p + 1) * per, block, above)
        at = pl.ds(rows - (p + 1) * size, size)
        for i, (src, dst) in enumerate(outs):
            for n in range(costs):
                pltpu.make_async_copy(src.at[at, n, :], dst.at[n, at], osem.at[i]).start()
    for i, (src, dst) in enumerate(outs):
        pltpu.make_async_copy(dst, dst, osem.at[i]).wait()


def solution(mesh):
    nlat, nlon = mesh.shape["lat"], mesh.shape["lon"]

    def body(forcing, depth_east, depth_north, surface_term, ocean_mask, cost_weights):
        costs, rows, cols = cost_weights.shape
        full, ringc = rows + 2 * HB, cols + 128
        f32 = jnp.float32
        dma = pltpu.SemaphoreType.DMA
        every = [(a, b) for a in range(nlat) for b in range(nlon) if a or b]
        stages = [every] if len(every) < 64 else [
            [(0, b) for b in range(1, nlon)], [(a, 0) for a in range(1, nlat)]]
        reduce_scratch = [
            ref for g in stages for ref in (
                pltpu.VMEM((1, 128), f32), pltpu.VMEM((len(g), 1, 128), f32),
                dma, dma)]
        rz = rows + HB
        shapes = (
            (DEG, rz, cols), (DEG - 1, rows, cols), (DEG - 1, rows, cols), (DEG - 1, rows, cols), (DEG, rz, cols),
            (ITERS, rows + HS + HW, costs, ringc), (ITERS - 1, rows, costs, cols),
            (5, rows, cols), (rz, cols), (NCOEF, costs, 128), (DEG + 1, costs, 128), (ITERS, costs, 128))
        hbm = pl.BlockSpec(memory_space=pltpu.HBM)
        vmem = pl.BlockSpec(memory_space=pltpu.VMEM)
        args = (forcing, depth_east, depth_north, surface_term, ocean_mask, cost_weights)
        mids = pl.pallas_call(
            functools.partial(kernel, nlat, nlon, stages),
            out_shape=[pltpu.VMEM(x, f32) for x in shapes],
            in_specs=[hbm] * 6,
            out_specs=[vmem] * len(shapes),
            scratch_shapes=[
                pltpu.VMEM((4, rows, cols), f32),
                pltpu.VMEM((rows, cols), jnp.int32),
                pltpu.VMEM((rows, costs, cols), f32),
                dma((3,)),
                pltpu.VMEM((rows, 128), f32),
                pltpu.VMEM((rows, 128), f32),
                *[pltpu.VMEM((full, 128), f32)] * 2,
                *[pltpu.VMEM((2 * HB, 128), f32)] * 2,
                *[pltpu.VMEM((4, HB, cols), f32)] * 4,
                *[pltpu.VMEM((HB, cols), jnp.int32)] * 4,
                pltpu.VMEM((HW, costs, cols), f32),
                pltpu.VMEM((HS, costs, cols), f32),
                *[pltpu.VMEM((rows // 8, costs, 128), f32)] * 2,
                *[pltpu.VMEM((rows // 8 + 2, costs, 128), f32)] * 2,
                pltpu.VMEM((2, rows + 4 * HB, ringc), f32),
                pltpu.VMEM((DEG - 1, rows, cols), f32),
                *[pltpu.VMEM((full, ringc), f32)] * 3,
                *[pltpu.VMEM((rows + 4 * HB, ringc), f32)] * 2,
                pltpu.VMEM((rows // 8 + 2, costs, 128), f32),
                dma((16,)),
                dma((16,)),
                pltpu.SemaphoreType.REGULAR((max(1, (max(nlat, nlon) - 1).bit_length() - 1),)),
                *reduce_scratch,
            ],
            compiler_params=pltpu.CompilerParams(
                collective_id=0, has_side_effects=True, vmem_limit_bytes=24 * 1024 * 1024
            ),
        )(*[pltpu.with_memory_space_constraint(x, pltpu.HBM) for x in args])
        out = (costs, rows, cols)
        return pl.pallas_call(
            adjoint_kernel,
            out_shape=[jax.ShapeDtypeStruct(out, f32)] * 3,
            in_specs=[vmem] * len(shapes),
            out_specs=[hbm] * 3,
            scratch_shapes=[
                pltpu.VMEM((ITERS - 1, rz, cols), f32),
                pltpu.VMEM((ITERS - 1, rows, cols), f32),
                pltpu.VMEM((ITERS, rz, cols), f32),
                *[pltpu.VMEM((rows, costs, cols), f32)] * 3,
                dma((3,)),
            ],
            compiler_params=pltpu.CompilerParams(vmem_limit_bytes=24 * 1024 * 1024),
        )(*[pltpu.with_memory_space_constraint(x, pltpu.VMEM) for x in mids])

    grid = P("lat", "lon")
    field = P(None, "lat", "lon")
    return jax.shard_map(
        body,
        mesh=mesh,
        in_specs=(grid, grid, grid, grid, grid, field),
        out_specs=(field, field, field),
        check_vma=False,
    )
```

```python
import functools

import jax
import jax.numpy as jnp
from jax import lax
from jax.experimental import pallas as pl
from jax.experimental.pallas import tpu as pltpu
from jax.sharding import PartitionSpec as P

ITERS = 6
MESH = pl.DeviceIdType.MESH
HB = 8
HS = 5
BLOCK = 8
GROUPED = 4
HC = 13
HW = 6
GROUP = 16
DEG = 2 * ITERS
CS, CC = 0, ITERS
CX = CC + ITERS
CH = CX + DEG - 1
CM = CH + DEG
NCOEF = CM + DEG


def coefficients(mu, proj):
    def gram(a, b):
        return 0.5 * (mu[a + b] + mu[abs(a - b)])

    h = {}
    for a in range(ITERS):
        for b in range(a, ITERS):
            h[a, b] = gram(a, b) - 0.5 * (gram(a, b + 1) + gram(a, abs(b - 1)))
    g, p = list(mu[:ITERS]), list(proj)
    low, inv = {}, []
    for i in range(ITERS):
        inv.append(1.0 / h[i, i])
        for j in range(i + 1, ITERS):
            low[j, i] = h[i, j] * inv[i]
        for j in range(i + 1, ITERS):
            for k in range(j, ITERS):
                h[j, k] = h[j, k] - low[j, i] * h[i, k]
            g[j] = g[j] - low[j, i] * g[i]
            p[j] = p[j] - low[j, i] * p[i]
    c, d = [None] * ITERS, [None] * ITERS
    for i in range(ITERS - 1, -1, -1):
        c[i], d[i] = g[i] * inv[i], p[i] * inv[i]
        for j in range(i + 1, ITERS):
            c[i] = c[i] - low[j, i] * c[j]
            d[i] = d[i] - low[j, i] * d[j]
    zero = jnp.zeros_like(c[0])
    cc = c + [zero, zero]
    res = [1.0 - c[0] + 0.5 * c[1], c[0] + 0.5 * cc[2] - c[1]]
    for j in range(2, ITERS + 1):
        res.append(0.5 * (cc[j - 1] + cc[j + 1]) - cc[j])
    bar = [zero] * DEG
    for a in range(ITERS):
        half = 0.5 * d[a]
        for j in range(ITERS + 1):
            t = half * res[j]
            bar[a + j] = bar[a + j] + t
            bar[abs(a - j)] = bar[abs(a - j)] + t
    return c, bar


def roll(x, shift, axis):
    return pltpu.roll(x, shift % x.shape[axis], axis)


def east(x):
    return roll(x, -1, 1)


def north(x):
    return roll(x, -1, 0)


def total_of(terms):
    acc = None
    for t in terms:
        acc = t if acc is None else acc + t
    return acc


def kernel(nlat, nlon, stages, f_hbm, de_hbm, dn_hbm, st_hbm, mk_hbm, w_hbm,
           un, ue, xe, xn, ww, v, ve, geo, dia, coef, us_side, vs_side,
           fields, mk_ref, w_ref, lsem,
           send_w, send_e, main, row_n, row_s, cor_n, cor_s, far_n, far_s, farc_n, farc_s,
           wrow_n, wrow_s, wsend_w, wsend_e, wmain, wcor_n, wcor_s,
           up, unn, e2r, n2r, rsr, e2w, n2w, comb, ssem, rsem, hello,
           *reduce_refs):
    lat, lon = lax.axis_index("lat"), lax.axis_index("lon")
    rows, costs, cols = w_ref.shape
    for i, src in enumerate((f_hbm, de_hbm, dn_hbm, st_hbm)):
        pltpu.make_async_copy(src, fields.at[i], lsem.at[0]).start()
    pltpu.make_async_copy(mk_hbm, mk_ref, lsem.at[1]).start()
    for n in range(costs):
        pltpu.make_async_copy(w_hbm.at[n], w_ref.at[:, n, :], lsem.at[2]).start()

    def loaded(i, ref):
        pltpu.make_async_copy(ref, ref, lsem.at[i]).wait()

    def peer(dlat, dlon):
        return (lax.rem(lat + dlat + nlat, nlat), lax.rem(lon + dlon + nlon, nlon))

    has_s, has_n = lat > 0, lat < nlat - 1

    def beside(r):
        return sorted({-r % nlon, 0, r % nlon})

    def greet(sem, r):
        for dlat, there in ((0, None), (-r, lat >= r), (r, lat < nlat - r)):
            def go(dlat=dlat):
                for b in beside(r):
                    if dlat or b:
                        pl.semaphore_signal(sem, inc=1, device_id=(lat + dlat, lax.rem(lon + b, nlon)),
                                            device_id_type=MESH)
            if there is None:
                go()
            elif r < nlat:
                pl.when(there)(go)

    def greeted(sem, r):
        lines = 1 + (lat >= r).astype(jnp.int32) + (lat < nlat - r).astype(jnp.int32)
        pl.semaphore_wait(sem, lines * len(beside(r)) - 1)

    barrier = pltpu.get_barrier_semaphore()
    rounds, radius = [], 1
    while radius < max(nlat - 1, nlon // 2):
        rounds.append(radius)
        radius *= 2
    greet(barrier, 1)

    @pl.when(lat == nlat - 1)
    def _():
        for ref in (row_n, cor_n, far_n, farc_n, wrow_n, wcor_n):
            ref[...] = jnp.zeros_like(ref)

    @pl.when(lat == 0)
    def _():
        for ref in (row_s, cor_s, far_s, farc_s, wrow_s, wcor_s):
            ref[...] = jnp.zeros_like(ref)

    loaded(0, fields.at[pl.ds(0, 4)])
    loaded(1, mk_ref)
    fields[4] = mk_ref[...].astype(jnp.float32)

    lane = lax.broadcasted_iota(jnp.int32, (rows, 128), 1)
    for ref, at, first in ((send_w, slice(0, 128), True), (send_e, slice(cols - 128, cols), False)):
        buf = jnp.zeros((rows, 128), jnp.float32)
        for i in range(5):
            pos = HC * i
            tile = fields[i, :, at]
            tile = roll(tile, pos if first else pos + HC, 1)
            buf = jnp.where((lane >= pos) & (lane < pos + HC), tile, buf)
        ref[...] = buf
    greeted(barrier, 1)
    if rounds:
        greet(hello.at[0], rounds[0])

    groups, pending = [], []

    def whole(i):
        ref = groups[i][0]
        return pltpu.make_async_remote_copy(src_ref=ref, dst_ref=ref, send_sem=ssem.at[i], recv_sem=rsem.at[i],
                                            device_id=peer(0, 1), device_id_type=MESH)

    def send(ref, side, parts):
        i = len(groups)
        groups.append((ref, side))
        pending.append((i, side, parts))

    def depart():
        for i, side, parts in pending:
            def go(i=i, parts=parts):
                for src, dst, dev in parts:
                    pltpu.make_async_remote_copy(src_ref=src, dst_ref=dst, send_sem=ssem.at[i], recv_sem=rsem.at[i],
                                                 device_id=dev, device_id_type=MESH).start()
            if side == 0:
                go()
            else:
                pl.when(has_s if side > 0 else has_n)(go)
        pending.clear()

    def arrive(span):
        for i in span:
            side = groups[i][1]
            if side == 0:
                whole(i).wait_recv()
            else:
                pl.when(has_n if side > 0 else has_s)(lambda i=i: whole(i).wait_recv())

    def sent(span):
        for i in span:
            side = groups[i][1]
            if side == 0:
                whole(i).wait_send()
            else:
                pl.when(has_s if side > 0 else has_n)(lambda i=i: whole(i).wait_send())

    lo, hi, lo2, hi2 = (pl.ds(i, HB) for i in (0, rows - HB, HB, rows - 2 * HB))

    def corners(to, side, at):
        send(to, side, [(send_w.at[at], to.at[0], peer(-side, -1)), (send_e.at[at], to.at[1], peer(-side, 1))])

    corners(cor_n, 1, lo)
    corners(cor_s, -1, hi)
    send(row_n, 1, [(fields.at[:, lo], row_n, peer(-1, 0))])
    send(row_s, -1, [(fields.at[:, hi], row_s, peer(1, 0))])
    send(main, 0, [(send_w, main.at[0], peer(0, -1)), (send_e, main.at[1], peer(0, 1))])
    depart()
    early = len(groups)
    corners(farc_n, 1, lo2)
    corners(farc_s, -1, hi2)
    send(far_n, 1, [(fields.at[:, lo2], far_n, peer(-1, 0))])
    send(far_s, -1, [(fields.at[:, hi2], far_s, peer(1, 0))])
    depart()
    late = len(groups)
    loaded(2, w_ref)
    send(wrow_n, 1, [(w_ref.at[pl.ds(0, HW)], wrow_n, peer(-1, 0))])
    send(wrow_s, -1, [(w_ref.at[pl.ds(rows - HS, HS)], wrow_s, peer(1, 0))])
    depart()
    lane8 = lax.broadcasted_iota(jnp.int32, (costs, 128), 1)
    sub8 = lax.broadcasted_iota(jnp.int32, (costs, 128), 0)
    for j in range(rows // 8):
        to_w, to_e = jnp.zeros((costs, 128), jnp.float32), jnp.zeros((costs, 128), jnp.float32)
        for g in range(8):
            at = GROUP * g
            first, last = w_ref[8 * j + g, :, :128], w_ref[8 * j + g, :, cols - 128:]
            to_w = jnp.where((lane8 >= at) & (lane8 < at + HW), roll(first, at, 1), to_w)
            end = at if g else 128
            to_e = jnp.where((lane8 >= end - HS) & (lane8 < end), roll(last, at, 1), to_e)
        wsend_w[j], wsend_e[j] = to_w, to_e
    strips = rows // 8
    for to, side, j in ((wcor_n, 1, 0), (wcor_s, -1, strips - 1)):
        send(to, side, [(wsend_w.at[j], to.at[0], peer(-side, -1)), (wsend_e.at[j], to.at[1], peer(-side, 1))])
    send(wmain, 0, [(wsend_w, wmain.at[0], peer(0, -1)), (wsend_e, wmain.at[1], peer(0, 1))])
    depart()
    for i in range(1, len(rounds)):
        greeted(hello.at[i - 1], rounds[i - 1])
        greet(hello.at[i], rounds[i])
    arrive(range(early))

    full = rows + 2 * HB
    def operator(mains, got_e, got_w):
        height = got_e.shape[0]
        lane = lax.broadcasted_iota(jnp.int32, (height, 128), 1)

        def padded(i):
            a = roll(got_e, -HC * i, 1)
            b = roll(got_w, 128 - HC - HC * i, 1)
            side = jnp.where(lane < HC, a, jnp.where(lane >= 128 - HC, b, 0.0))
            return jnp.concatenate([mains(i), side], axis=1)

        wet = padded(4)
        ex = padded(1) * wet * east(wet)
        ey = padded(2) * wet * north(wet)
        base = wet * padded(3) + 1.0 - wet
        diag = base + ex + roll(ex, 1, 1) + ey + roll(ey, 1, 0)
        rs = lax.rsqrt(diag)
        rs = rs * (1.5 - 0.5 * diag * rs * rs)
        rs_e, rs_n = rs * east(rs), rs * north(rs)
        return wet, rs, rs_e, rs_n, 2.0 * ex * rs_e, 2.0 * ey * rs_n, rs * padded(0)

    def stacked(order):
        return lambda i: jnp.concatenate([ref[i] if at is None else ref[i, at] for ref, at in order], axis=0)

    def strip(j):
        return jnp.concatenate([main[j], cor_n[j], cor_s[j]], axis=0)

    wet, rs, rs_e, rs_n, e2, n2, u0 = operator(
        stacked(((fields, None), (row_n, None), (row_s, None))), strip(0), strip(1))
    e2r[...], n2r[...], rsr[...] = e2, n2, rs
    rz = rows + HB

    lane_r = lax.broadcasted_iota(jnp.int32, (rows, 128), 1)
    row_r = lax.broadcasted_iota(jnp.int32, (rows, 128), 0)

    def to_lanes(column):
        return jnp.broadcast_to(jnp.sum(jnp.where(lane_r == row_r, column, 0.0), axis=0, keepdims=True), (costs, 128))

    def keep(k, u):
        un[k] = u[:rz, :cols]
        us_side[k] = to_lanes(u[:rows, cols:cols + 1])

    def step(k, x, prev, prev2, le, ln, e2, n2):
        s = e2 * le + roll(e2 * prev, 1, 1) + n2 * ln + roll(n2 * prev, 1, 0)
        return s if k == 1 else s - (prev2 + prev2 if k == 2 else prev2)

    us = [u0]
    for k in range(1, ITERS + 1):
        le, ln = east(us[k - 1]), north(us[k - 1])
        keep(k - 1, us[k - 1])
        ue[k - 1], unn[k - 1] = le[:rows, :cols], ln[:rows, :cols]
        us.append(step(k, None, us[k - 1], us[k - 2] if k > 1 else None, le, ln, e2, n2))
    keep(ITERS, us[ITERS])

    inner = [u[:rows, :cols] for u in us]
    rs_in = rs[:rows, :cols]

    mom = ITERS * costs

    def fold(field):
        return total_of(field[i:i + 8, j:j + 128] for i in range(0, rows, 8) for j in range(0, cols, 128))

    mine = jnp.zeros((costs, 128), jnp.float32)
    for k in range(ITERS):
        for m, field in ((2 * k, inner[k] * inner[k]), (2 * k + 1, inner[k] * inner[k + 1])):
            mine = jnp.where(lane8 == mom + m, jnp.sum(fold(field), axis=1, keepdims=True), mine)
    proj = [None] * ITERS
    for r in range(rows):
        wr = w_ref[r] * rsr[r:r + 1, :cols]
        for k in range(ITERS):
            pr = wr * un[k, r:r + 1, :]
            proj[k] = pr if proj[k] is None else proj[k] + pr
    for k in range(ITERS):
        line = total_of(proj[k][:, j:j + 128] for j in range(0, cols, 128))
        mine = jnp.where(lane8 == costs * k + sub8, jnp.sum(line, axis=1, keepdims=True), mine)
    mine = jnp.sum(mine, axis=0, keepdims=True)

    def start(stage, value):
        mailbox, got, ss, rv = reduce_refs[4 * stage:4 * stage + 4]
        mailbox[...] = value
        for i, (a, b) in enumerate(stages[stage]):
            pltpu.make_async_remote_copy(src_ref=mailbox, dst_ref=got.at[i], send_sem=ss, recv_sem=rv,
                                         device_id=peer(a, b), device_id_type=MESH).start()
        all_of = pltpu.make_async_remote_copy(src_ref=got, dst_ref=got, send_sem=ss, recv_sem=rv,
                                              device_id=peer(0, 1), device_id_type=MESH)
        waits.append(all_of)
        return all_of

    def finish(stage, group, value):
        group.wait_recv()
        got = reduce_refs[4 * stage + 1]
        parts = [value] + [got[i] for i in range(len(stages[stage]))]
        while len(parts) > 1:
            parts = [sum(parts[i:i + 2][1:], parts[i]) for i in range(0, len(parts), 2)]
        return parts[0]

    waits = []
    if rounds:
        greeted(hello.at[len(rounds) - 1], rounds[-1])
    group = start(0, mine)

    arrive(range(early, late))

    low, high = slice(rows - HB, rows), slice(0, HB)

    def strip_band(j):
        return jnp.concatenate([main[j, low], cor_n[j], farc_n[j], farc_s[j], cor_s[j], main[j, high]], axis=0)

    _, _, _, _, e2b, n2b, b0 = operator(
        stacked(((fields, low), (row_n, None), (far_n, None), (far_s, None), (row_s, None), (fields, high))),
        strip_band(0), strip_band(1))
    band = [b0]
    for k in range(1, ITERS + 1):
        band.append(step(k, None, band[-1], band[-2] if k > 1 else None, east(band[-1]), north(band[-1]), e2b, n2b))

    def joined(main, halo):
        return jnp.concatenate([main[:rows], halo[HB:5 * HB]], axis=0)

    e2w[...], n2w[...] = joined(e2, e2b), joined(n2, n2b)
    for k in (ITERS - 1, ITERS):
        up[k % 2] = joined(us[k], band[k])
    for k in range(ITERS + 1, DEG):
        prev, prev2 = up[(k - 1) % 2], up[k % 2]
        le, ln = east(prev), north(prev)
        ue[k - 1], unn[k - 1] = le[:rows, :cols], ln[:rows, :cols]
        x = step(k, None, prev, prev2, le, ln, e2w[...], n2w[...])
        keep(k, x)
        up[k % 2] = x

    wet_in = wet[:rows, :cols]
    me = wet_in * east(wet)[:rows, :cols]
    mn = wet_in * north(wet)[:rows, :cols]
    geo[0], geo[1] = me, mn
    geo[2] = me * rs_e[:rows, :cols]
    geo[3] = mn * rs_n[:rows, :cols]
    geo[4] = rs_in
    rs_z = rsr[:rz, :cols]
    dia[...] = -0.5 * rs_z * rs_z
    rs_c = rsr[:rows, cols:cols + 1]
    us_side[DEG] = to_lanes(-0.5 * rs_c * rs_c)

    def products(t, carry):
        at = pl.ds(pl.multiple_of(t * 8, 8), 8)
        u = [un[k, at, :] for k in range(DEG)]
        for s in range(DEG):
            acc = None
            for a in range((s + 1) // 2):
                pr = u[a] * u[s - a]
                acc = pr if acc is None else acc + pr
            acc = acc + acc if acc is not None else None
            if s % 2 == 0:
                sq = u[s // 2] * u[s // 2]
                acc = sq if acc is None else acc + sq
            ww[s, at, :] = acc
        return carry

    def cross(t, carry):
        at = pl.ds(pl.multiple_of(t * 8, 8), 8)
        for src, dst in ((ue, xe), (unn, xn)):
            for s in range(DEG - 1):
                acc = None
                for a in range(s + 1):
                    pr = un[a, at, :cols] * src[s - a, at, :]
                    acc = pr if acc is None else acc + pr
                dst[s, at, :] = acc
        return carry

    lax.fori_loop(0, rz // 8, products, 0)
    lax.fori_loop(0, rows // 8, cross, 0)

    arrive(range(late, len(groups)))

    for j in range(strips + 2):
        a, b = ((wmain.at[0, j], wmain.at[1, j]) if j < strips else
                (wcor_n.at[0], wcor_n.at[1]) if j == strips else (wcor_s.at[0], wcor_s.at[1]))
        comb[j] = jnp.where(lane8 % GROUP < HW, a[...], b[...])

    def ring_row(r):
        return r if r >= 0 else full + r

    def line(ref, r):
        q = ring_row(r)
        return ref[q:q + 1, :]

    for r in range(-HS, rows + HW):
        if r < 0:
            block, packed, g = wrow_s[r + HS], comb[strips + 1], 8 + r
        elif r >= rows:
            block, packed, g = wrow_n[r - rows], comb[strips], r - rows
        else:
            block, packed, g = w_ref[r], comb[r // 8], r % 8
        side_r = roll(packed, -GROUP * g, 1)
        v[0, r + HS] = line(rsr, r) * jnp.concatenate([block, side_r], axis=1)

    for k in range(1, ITERS):
        for r in range(k - HS, rows + HW - k):
            x = v[k - 1, r + HS]
            e = line(e2r, r)
            le = east(x)
            y = e * le + roll(e * x, 1, 1) + line(n2r, r) * v[k - 1, r + HS + 1] + line(n2r, r - 1) * v[k - 1, r + HS - 1]
            if k > 1:
                before = v[k - 2, r + HS]
                y = y - (before + before if k == 2 else before)
            v[k, r + HS] = y
            if 0 <= r < rows:
                ve[k - 1, r] = le[:, :cols]
    for k in range(ITERS):
        acc = jnp.zeros((costs, 128), jnp.float32)
        for r in range(rows):
            acc = jnp.where(lane8 == r, roll(v[k, r + HS, :, cols:], r, 1), acc)
        vs_side[k] = acc

    total = finish(0, group, mine)
    for stage in range(1, len(stages)):
        total = finish(stage, start(stage, total), total)

    tot8 = jnp.broadcast_to(total, (costs, 128))
    def pick(index):
        return jnp.broadcast_to(
            jnp.sum(jnp.where(lane8 == index, tot8, 0.0), axis=1, keepdims=True), (costs, 128))

    proj = [pick(k * costs + sub8) * (0.5 if k else 1.0) for k in range(ITERS)]
    raw = [pick(mom + m) * (0.5 if m == 1 else 0.25 if m else 1.0) for m in range(DEG)]
    mu = [raw[0], raw[1]]
    for k in range(1, ITERS):
        mu += [2.0 * raw[2 * k] - raw[0], 2.0 * raw[2 * k + 1] - raw[1]]
    c, bar = coefficients(mu, proj)
    zero = jnp.zeros_like(c[0])
    acc = [zero] * (ITERS + 2)
    for m in range(ITERS - 1, -1, -1):
        acc[m] = c[m] + acc[m + 2]
    tail = [zero] * (DEG + 2)
    for m in range(DEG - 1, -1, -1):
        tail[m] = bar[m] + tail[m + 2]
    for m in range(ITERS):
        coef[CS + m] = acc[m]
        coef[CC + m] = 0.5 * c[m] if m else c[m]
    for s in range(DEG - 1):
        coef[CX + s] = 2.0 * tail[s + 1]
    for s in range(DEG):
        coef[CH + s] = tail[s] + tail[s + 2] if s else 2.0 * tail[0]
        coef[CM + s] = bar[s] if s else 2.0 * bar[0]
    sent(range(len(groups)))
    for c in waits:
        c.wait_send()


def adjoint_kernel(un, ue, xe, xn, ww, v, ve, geo, dia, coef, us_side, vs_side,
                   fa_hbm, ge_hbm, gn_hbm, y, ye, z, fa_ref, ge_ref, gn_ref, osem):
    rows, costs, cols = fa_ref.shape
    rz = dia.shape[0]

    outs = ((fa_ref, fa_hbm), (ge_ref, ge_hbm), (gn_ref, gn_hbm))

    def factor(i, width, at=None):
        c = coef[i] if at is None else coef[i, at:at + 1]
        return jnp.concatenate([c] * (width // 128), axis=1)

    def vectors(u, width, at):
        return [total_of(factor(CS + a + b + 1, width, at) * u[b] for b in range(ITERS - 1 - a))
                for a in range(-1, ITERS - 1)]

    def diagonal(ys, u, width, at):
        out = [ys[0] + ys[2] + factor(CC, width, at) * u[0]]
        return out + [ys[a] + ys[a + 2] if a + 2 < len(ys) else ys[a] for a in range(1, ITERS)]

    def combine(t, carry):
        at = pl.ds(pl.multiple_of(t * 8, 8), 8)
        u = [un[k, at, :] for k in range(ITERS)]
        ys = vectors(u, cols, 0)
        for a, f in enumerate(diagonal(ys, u, cols, 0)):
            z[a, at, :] = f
        for a in range(ITERS - 1):
            y[a, at, :] = ys[a + 1]
        return carry

    def combine_east(t, carry):
        at = pl.ds(pl.multiple_of(t * 8, 8), 8)
        u = [ue[k, at, :] for k in range(ITERS - 1)]
        for a in range(ITERS - 1):
            ye[a, at, :] = total_of(factor(CS + a + b + 1, cols, 0) * u[b] for b in range(ITERS - 1 - a))
        return carry

    lax.fori_loop(0, rz // 8, combine, 0)
    lax.fori_loop(0, rows // 8, combine_east, 0)
    u = [us_side[k] for k in range(DEG)]
    zs = diagonal(vectors(u, 128, None), u, 128, None)
    side = total_of(zs[a] * vs_side[a] for a in range(ITERS))
    for s in range(DEG):
        side = side + coef[CH + s] * total_of(u[a] * u[s - a] for a in range(s + 1))
    side = side * us_side[DEG]
    lane_c = lax.broadcasted_iota(jnp.int32, (costs, cols), 1)

    def line(ref, *at):
        return ref[(*at[:-1], pl.ds(at[-1], 1), slice(None))]

    def diag_of(r):
        acc = total_of(line(z, a, r) * v[a, r + HS, :, :cols] for a in range(ITERS))
        for s in range(DEG):
            acc = acc + factor(CH + s, cols) * line(ww, s, r)
        return acc * line(dia, r)

    def rows_of(rs, above):
        def add(acc, term):
            return term if acc is None else acc + term

        ge, gn, fa, db = ([None] * len(rs) for _ in range(4))
        for i, r in enumerate(rs):
            for a in range(ITERS):
                x = v[a, r + HS, :, :cols]
                db[i] = add(db[i], x * line(z, a, r))
                fa[i] = add(fa[i], x * factor(CC + a, cols))
                if a < ITERS - 1:
                    here = line(y, a, r)
                    ge[i] = add(ge[i], x * line(ye, a, r) + ve[a, r] * here)
                    gn[i] = add(gn[i], x * line(y, a, r + 1) + v[a, r + HS + 1, :, :cols] * here)
        for first, count, acc, field in ((CH, DEG, db, ww), (CX, DEG - 1, ge, xe), (CX, DEG - 1, gn, xn), (CM, DEG, fa, un)):
            for s in range(count):
                c = factor(first + s, cols)
                for i, r in enumerate(rs):
                    acc[i] = acc[i] + c * line(field, s, r)
        for i, r in enumerate(rs):
            d = db[i] * line(dia, r)
            end = jnp.concatenate([pltpu.roll(side, 127 - r, 1)] * (cols // 128), axis=1)
            d_e = jnp.where(lane_c == cols - 1, end, east(d))
            fa_ref[r] = line(geo, 4, r) * fa[i]
            ge_ref[r] = line(geo, 2, r) * ge[i] + line(geo, 0, r) * (d + d_e)
            gn_ref[r] = line(geo, 3, r) * gn[i] + line(geo, 1, r) * (d + above)
            above = d
        return above

    parts = 2
    size = rows // parts

    def block(i, above):
        first = rows - (i + 1) * BLOCK
        for j in range(BLOCK - 1, -1, -GROUPED):
            above = rows_of([first + j - i for i in range(GROUPED)], above)
        return above

    above = diag_of(rows)
    per = size // BLOCK
    for p in range(parts):
        above = lax.fori_loop(p * per, (p + 1) * per, block, above)
        at = pl.ds(rows - (p + 1) * size, size)
        for i, (src, dst) in enumerate(outs):
            for n in range(costs):
                pltpu.make_async_copy(src.at[at, n, :], dst.at[n, at], osem.at[i]).start()
    for i, (src, dst) in enumerate(outs):
        pltpu.make_async_copy(dst, dst, osem.at[i]).wait()


def solution(mesh):
    nlat, nlon = mesh.shape["lat"], mesh.shape["lon"]

    def body(forcing, depth_east, depth_north, surface_term, ocean_mask, cost_weights):
        costs, rows, cols = cost_weights.shape
        full, ringc = rows + 2 * HB, cols + 128
        f32 = jnp.float32
        dma = pltpu.SemaphoreType.DMA
        every = [(a, b) for a in range(nlat) for b in range(nlon) if a or b]
        stages = [every] if len(every) < 64 else [
            [(0, b) for b in range(1, nlon)], [(a, 0) for a in range(1, nlat)]]
        reduce_scratch = [
            ref for g in stages for ref in (
                pltpu.VMEM((1, 128), f32), pltpu.VMEM((len(g), 1, 128), f32),
                dma, dma)]
        rz = rows + HB
        shapes = (
            (DEG, rz, cols), (DEG - 1, rows, cols), (DEG - 1, rows, cols), (DEG - 1, rows, cols), (DEG, rz, cols),
            (ITERS, rows + HS + HW, costs, ringc), (ITERS - 1, rows, costs, cols),
            (5, rows, cols), (rz, cols), (NCOEF, costs, 128), (DEG + 1, costs, 128), (ITERS, costs, 128))
        hbm = pl.BlockSpec(memory_space=pltpu.HBM)
        vmem = pl.BlockSpec(memory_space=pltpu.VMEM)
        args = (forcing, depth_east, depth_north, surface_term, ocean_mask, cost_weights)
        mids = pl.pallas_call(
            functools.partial(kernel, nlat, nlon, stages),
            out_shape=[pltpu.VMEM(x, f32) for x in shapes],
            in_specs=[hbm] * 6,
            out_specs=[vmem] * len(shapes),
            scratch_shapes=[
                pltpu.VMEM((5, rows, cols), f32),
                pltpu.VMEM((rows, cols), jnp.int32),
                pltpu.VMEM((rows, costs, cols), f32),
                dma((3,)),
                pltpu.VMEM((rows, 128), f32),
                pltpu.VMEM((rows, 128), f32),
                pltpu.VMEM((2, rows, 128), f32),
                *[pltpu.VMEM((5, HB, cols), f32)] * 2,
                *[pltpu.VMEM((2, HB, 128), f32)] * 2,
                *[pltpu.VMEM((5, HB, cols), f32)] * 2,
                *[pltpu.VMEM((2, HB, 128), f32)] * 2,
                pltpu.VMEM((HW, costs, cols), f32),
                pltpu.VMEM((HS, costs, cols), f32),
                *[pltpu.VMEM((rows // 8, costs, 128), f32)] * 2,
                pltpu.VMEM((2, rows // 8, costs, 128), f32),
                *[pltpu.VMEM((2, costs, 128), f32)] * 2,
                pltpu.VMEM((2, rows + 4 * HB, ringc), f32),
                pltpu.VMEM((DEG - 1, rows, cols), f32),
                *[pltpu.VMEM((full, ringc), f32)] * 3,
                *[pltpu.VMEM((rows + 4 * HB, ringc), f32)] * 2,
                pltpu.VMEM((rows // 8 + 2, costs, 128), f32),
                dma((14,)),
                dma((14,)),
                pltpu.SemaphoreType.REGULAR((max(1, (max(nlat - 1, nlon // 2) - 1).bit_length()),)),
                *reduce_scratch,
            ],
            compiler_params=pltpu.CompilerParams(
                collective_id=0, has_side_effects=True, vmem_limit_bytes=24 * 1024 * 1024
            ),
        )(*[pltpu.with_memory_space_constraint(x, pltpu.HBM) for x in args])
        out = (costs, rows, cols)
        return pl.pallas_call(
            adjoint_kernel,
            out_shape=[jax.ShapeDtypeStruct(out, f32)] * 3,
            in_specs=[vmem] * len(shapes),
            out_specs=[hbm] * 3,
            scratch_shapes=[
                pltpu.VMEM((ITERS - 1, rz, cols), f32),
                pltpu.VMEM((ITERS - 1, rows, cols), f32),
                pltpu.VMEM((ITERS, rz, cols), f32),
                *[pltpu.VMEM((rows, costs, cols), f32)] * 3,
                dma((3,)),
            ],
            compiler_params=pltpu.CompilerParams(vmem_limit_bytes=24 * 1024 * 1024),
        )(*[pltpu.with_memory_space_constraint(x, pltpu.VMEM) for x in mids])

    grid = P("lat", "lon")
    field = P(None, "lat", "lon")
    return jax.shard_map(
        body,
        mesh=mesh,
        in_specs=(grid, grid, grid, grid, grid, field),
        out_specs=(field, field, field),
        check_vma=False,
    )
```

```python
import functools

import jax
import jax.numpy as jnp
from jax import lax
from jax.experimental import pallas as pl
from jax.experimental.pallas import tpu as pltpu
from jax.sharding import PartitionSpec as P

ITERS = 6
MESH = pl.DeviceIdType.MESH
HB = 8
HS = 5
BLOCK = 8
GROUPED = 4
HC = 13
HW = 6
GROUP = 16
DEG = 2 * ITERS
CS, CC = 0, ITERS
CX = CC + ITERS
CH = CX + DEG - 1
CM = CH + DEG
NCOEF = CM + DEG


def coefficients(mu, proj):
    def gram(a, b):
        return 0.5 * (mu[a + b] + mu[abs(a - b)])

    h = {}
    for a in range(ITERS):
        for b in range(a, ITERS):
            h[a, b] = gram(a, b) - 0.5 * (gram(a, b + 1) + gram(a, abs(b - 1)))
    g, p = list(mu[:ITERS]), list(proj)
    low, inv = {}, []
    for i in range(ITERS):
        inv.append(1.0 / h[i, i])
        for j in range(i + 1, ITERS):
            low[j, i] = h[i, j] * inv[i]
        for j in range(i + 1, ITERS):
            for k in range(j, ITERS):
                h[j, k] = h[j, k] - low[j, i] * h[i, k]
            g[j] = g[j] - low[j, i] * g[i]
            p[j] = p[j] - low[j, i] * p[i]
    c, d = [None] * ITERS, [None] * ITERS
    for i in range(ITERS - 1, -1, -1):
        c[i], d[i] = g[i] * inv[i], p[i] * inv[i]
        for j in range(i + 1, ITERS):
            c[i] = c[i] - low[j, i] * c[j]
            d[i] = d[i] - low[j, i] * d[j]
    zero = jnp.zeros_like(c[0])
    cc = c + [zero, zero]
    res = [1.0 - c[0] + 0.5 * c[1], c[0] + 0.5 * cc[2] - c[1]]
    for j in range(2, ITERS + 1):
        res.append(0.5 * (cc[j - 1] + cc[j + 1]) - cc[j])
    bar = [zero] * DEG
    for a in range(ITERS):
        half = 0.5 * d[a]
        for j in range(ITERS + 1):
            t = half * res[j]
            bar[a + j] = bar[a + j] + t
            bar[abs(a - j)] = bar[abs(a - j)] + t
    return c, bar


def roll(x, shift, axis):
    return pltpu.roll(x, shift % x.shape[axis], axis)


def east(x):
    return roll(x, -1, 1)


def north(x):
    return roll(x, -1, 0)


def total_of(terms):
    acc = None
    for t in terms:
        acc = t if acc is None else acc + t
    return acc


def kernel(nlat, nlon, stages, f_hbm, de_hbm, dn_hbm, st_hbm, mk_hbm, w_hbm,
           un, ue, xe, xn, ww, v, ve, geo, dia, coef, us_side, vs_side,
           fields, mk_ref, w_ref, lsem,
           send_w, send_e, main, row_n, row_s, cor_n, cor_s, far_n, far_s, farc_n, farc_s,
           wrow_n, wrow_s, wsend_w, wsend_e, wmain, wcor_n, wcor_s,
           up, unn, e2r, n2r, rsr, comb, ssem, rsem, hello,
           *reduce_refs):
    lat, lon = lax.axis_index("lat"), lax.axis_index("lon")
    rows, costs, cols = w_ref.shape
    for i, src in enumerate((f_hbm, de_hbm, dn_hbm, st_hbm)):
        pltpu.make_async_copy(src, fields.at[i], lsem.at[0]).start()
    pltpu.make_async_copy(mk_hbm, mk_ref, lsem.at[1]).start()
    for n in range(costs):
        pltpu.make_async_copy(w_hbm.at[n], w_ref.at[:, n, :], lsem.at[2]).start()

    def loaded(i, ref):
        pltpu.make_async_copy(ref, ref, lsem.at[i]).wait()

    def peer(dlat, dlon):
        return (lax.rem(lat + dlat + nlat, nlat), lax.rem(lon + dlon + nlon, nlon))

    has_s, has_n = lat > 0, lat < nlat - 1

    def beside(r):
        return sorted({-r % nlon, 0, r % nlon})

    def greet(sem, r):
        for dlat, there in ((0, None), (-r, lat >= r), (r, lat < nlat - r)):
            def go(dlat=dlat):
                for b in beside(r):
                    if dlat or b:
                        pl.semaphore_signal(sem, inc=1, device_id=(lat + dlat, lax.rem(lon + b, nlon)),
                                            device_id_type=MESH)
            if there is None:
                go()
            elif r < nlat:
                pl.when(there)(go)

    def greeted(sem, r):
        lines = 1 + (lat >= r).astype(jnp.int32) + (lat < nlat - r).astype(jnp.int32)
        pl.semaphore_wait(sem, lines * len(beside(r)) - 1)

    barrier = pltpu.get_barrier_semaphore()
    rounds, radius = [], 1
    while radius < max(nlat - 1, nlon // 2):
        rounds.append(radius)
        radius *= 2
    greet(barrier, 1)

    @pl.when(lat == nlat - 1)
    def _():
        for ref in (row_n, cor_n, far_n, farc_n, wrow_n, wcor_n):
            ref[...] = jnp.zeros_like(ref)

    @pl.when(lat == 0)
    def _():
        for ref in (row_s, cor_s, far_s, farc_s, wrow_s, wcor_s):
            ref[...] = jnp.zeros_like(ref)

    loaded(0, fields.at[pl.ds(0, 4)])
    loaded(1, mk_ref)
    fields[4] = mk_ref[...].astype(jnp.float32)

    lane = lax.broadcasted_iota(jnp.int32, (rows, 128), 1)
    for ref, at, first in ((send_w, slice(0, 128), True), (send_e, slice(cols - 128, cols), False)):
        buf = jnp.zeros((rows, 128), jnp.float32)
        for i in range(5):
            pos = HC * i
            tile = fields[i, :, at]
            tile = roll(tile, pos if first else pos + HC, 1)
            buf = jnp.where((lane >= pos) & (lane < pos + HC), tile, buf)
        ref[...] = buf
    greeted(barrier, 1)
    if rounds:
        greet(hello.at[0], rounds[0])

    groups, pending = [], []

    def whole(i):
        ref = groups[i][0]
        return pltpu.make_async_remote_copy(src_ref=ref, dst_ref=ref, send_sem=ssem.at[i], recv_sem=rsem.at[i],
                                            device_id=peer(0, 1), device_id_type=MESH)

    def send(ref, side, parts):
        i = len(groups)
        groups.append((ref, side))
        pending.append((i, side, parts))

    def depart():
        for i, side, parts in pending:
            def go(i=i, parts=parts):
                for src, dst, dev in parts:
                    pltpu.make_async_remote_copy(src_ref=src, dst_ref=dst, send_sem=ssem.at[i], recv_sem=rsem.at[i],
                                                 device_id=dev, device_id_type=MESH).start()
            if side == 0:
                go()
            else:
                pl.when(has_s if side > 0 else has_n)(go)
        pending.clear()

    def arrive(span):
        for i in span:
            side = groups[i][1]
            if side == 0:
                whole(i).wait_recv()
            else:
                pl.when(has_n if side > 0 else has_s)(lambda i=i: whole(i).wait_recv())

    def sent(span):
        for i in span:
            side = groups[i][1]
            if side == 0:
                whole(i).wait_send()
            else:
                pl.when(has_s if side > 0 else has_n)(lambda i=i: whole(i).wait_send())

    lo, hi, lo2, hi2 = (pl.ds(i, HB) for i in (0, rows - HB, HB, rows - 2 * HB))

    def corners(to, side, at):
        send(to, side, [(send_w.at[at], to.at[0], peer(-side, -1)), (send_e.at[at], to.at[1], peer(-side, 1))])

    corners(cor_n, 1, lo)
    corners(cor_s, -1, hi)
    send(row_n, 1, [(fields.at[:, lo], row_n, peer(-1, 0))])
    send(row_s, -1, [(fields.at[:, hi], row_s, peer(1, 0))])
    send(main, 0, [(send_w, main.at[0], peer(0, -1)), (send_e, main.at[1], peer(0, 1))])
    depart()
    early = len(groups)
    corners(farc_n, 1, lo2)
    corners(farc_s, -1, hi2)
    send(far_n, 1, [(fields.at[:, lo2], far_n, peer(-1, 0))])
    send(far_s, -1, [(fields.at[:, hi2], far_s, peer(1, 0))])
    depart()
    late = len(groups)
    loaded(2, w_ref)
    send(wrow_n, 1, [(w_ref.at[pl.ds(0, HW)], wrow_n, peer(-1, 0))])
    send(wrow_s, -1, [(w_ref.at[pl.ds(rows - HS, HS)], wrow_s, peer(1, 0))])
    depart()
    lane8 = lax.broadcasted_iota(jnp.int32, (costs, 128), 1)
    sub8 = lax.broadcasted_iota(jnp.int32, (costs, 128), 0)
    for j in range(rows // 8):
        to_w, to_e = jnp.zeros((costs, 128), jnp.float32), jnp.zeros((costs, 128), jnp.float32)
        for g in range(8):
            at = GROUP * g
            first, last = w_ref[8 * j + g, :, :128], w_ref[8 * j + g, :, cols - 128:]
            to_w = jnp.where((lane8 >= at) & (lane8 < at + HW), roll(first, at, 1), to_w)
            end = at if g else 128
            to_e = jnp.where((lane8 >= end - HS) & (lane8 < end), roll(last, at, 1), to_e)
        wsend_w[j], wsend_e[j] = to_w, to_e
    strips = rows // 8
    for to, side, j in ((wcor_n, 1, 0), (wcor_s, -1, strips - 1)):
        send(to, side, [(wsend_w.at[j], to.at[0], peer(-side, -1)), (wsend_e.at[j], to.at[1], peer(-side, 1))])
    send(wmain, 0, [(wsend_w, wmain.at[0], peer(0, -1)), (wsend_e, wmain.at[1], peer(0, 1))])
    depart()
    for i in range(1, len(rounds)):
        greeted(hello.at[i - 1], rounds[i - 1])
        greet(hello.at[i], rounds[i])
    arrive(range(early))

    full = rows + 2 * HB
    def operator(mains, got_e, got_w):
        height = got_e.shape[0]
        lane = lax.broadcasted_iota(jnp.int32, (height, 128), 1)

        def padded(i):
            a = roll(got_e, -HC * i, 1)
            b = roll(got_w, 128 - HC - HC * i, 1)
            side = jnp.where(lane < HC, a, jnp.where(lane >= 128 - HC, b, 0.0))
            return jnp.concatenate([mains(i), side], axis=1)

        wet = padded(4)
        ex = padded(1) * wet * east(wet)
        ey = padded(2) * wet * north(wet)
        base = wet * padded(3) + 1.0 - wet
        diag = base + ex + roll(ex, 1, 1) + ey + roll(ey, 1, 0)
        rs = lax.rsqrt(diag)
        rs = rs * (1.5 - 0.5 * diag * rs * rs)
        rs_e, rs_n = rs * east(rs), rs * north(rs)
        return wet, rs, rs_e, rs_n, 2.0 * ex * rs_e, 2.0 * ey * rs_n, rs * padded(0)

    def stacked(order):
        return lambda i: jnp.concatenate([ref[i] if at is None else ref[i, at] for ref, at in order], axis=0)

    def strip(j):
        return jnp.concatenate([main[j], cor_n[j], cor_s[j]], axis=0)

    wet, rs, rs_e, rs_n, e2, n2, u0 = operator(
        stacked(((fields, None), (row_n, None), (row_s, None))), strip(0), strip(1))
    e2r[...], n2r[...], rsr[...] = e2, n2, rs
    rz = rows + HB

    lane_r = lax.broadcasted_iota(jnp.int32, (rows, 128), 1)
    row_r = lax.broadcasted_iota(jnp.int32, (rows, 128), 0)

    def to_lanes(column):
        return jnp.broadcast_to(jnp.sum(jnp.where(lane_r == row_r, column, 0.0), axis=0, keepdims=True), (costs, 128))

    def keep(k, u):
        un[k] = u[:rz, :cols]
        us_side[k] = to_lanes(u[:rows, cols:cols + 1])

    def step(k, x, prev, prev2, le, ln, e2, n2):
        s = e2 * le + roll(e2 * prev, 1, 1) + n2 * ln + roll(n2 * prev, 1, 0)
        return s if k == 1 else s - (prev2 + prev2 if k == 2 else prev2)

    us = [u0]
    for k in range(1, ITERS + 1):
        le, ln = east(us[k - 1]), north(us[k - 1])
        keep(k - 1, us[k - 1])
        ue[k - 1], unn[k - 1] = le[:rows, :cols], ln[:rows, :cols]
        us.append(step(k, None, us[k - 1], us[k - 2] if k > 1 else None, le, ln, e2, n2))
    keep(ITERS, us[ITERS])

    inner = [u[:rows, :cols] for u in us]
    rs_in = rs[:rows, :cols]

    mom = ITERS * costs

    def fold(field):
        return total_of(field[i:i + 8, j:j + 128] for i in range(0, rows, 8) for j in range(0, cols, 128))

    mine = jnp.zeros((costs, 128), jnp.float32)
    for k in range(ITERS):
        for m, field in ((2 * k, inner[k] * inner[k]), (2 * k + 1, inner[k] * inner[k + 1])):
            mine = jnp.where(lane8 == mom + m, jnp.sum(fold(field), axis=1, keepdims=True), mine)
    proj = [None] * ITERS
    for r in range(rows):
        wr = w_ref[r] * rsr[r:r + 1, :cols]
        for k in range(ITERS):
            pr = wr * un[k, r:r + 1, :]
            proj[k] = pr if proj[k] is None else proj[k] + pr
    for k in range(ITERS):
        line = total_of(proj[k][:, j:j + 128] for j in range(0, cols, 128))
        mine = jnp.where(lane8 == costs * k + sub8, jnp.sum(line, axis=1, keepdims=True), mine)
    mine = jnp.sum(mine, axis=0, keepdims=True)

    def start(stage, value):
        mailbox, got, ss, rv = reduce_refs[4 * stage:4 * stage + 4]
        mailbox[...] = value
        for i, (a, b) in enumerate(stages[stage]):
            pltpu.make_async_remote_copy(src_ref=mailbox, dst_ref=got.at[i], send_sem=ss, recv_sem=rv,
                                         device_id=peer(a, b), device_id_type=MESH).start()
        all_of = pltpu.make_async_remote_copy(src_ref=got, dst_ref=got, send_sem=ss, recv_sem=rv,
                                              device_id=peer(0, 1), device_id_type=MESH)
        waits.append(all_of)
        return all_of

    def finish(stage, group, value):
        group.wait_recv()
        got = reduce_refs[4 * stage + 1]
        parts = [value] + [got[i] for i in range(len(stages[stage]))]
        while len(parts) > 1:
            parts = [sum(parts[i:i + 2][1:], parts[i]) for i in range(0, len(parts), 2)]
        return parts[0]

    waits = []
    if rounds:
        greeted(hello.at[len(rounds) - 1], rounds[-1])
    group = start(0, mine)

    arrive(range(early, late))

    low, high = slice(rows - HB, rows), slice(0, HB)

    def strip_band(j):
        return jnp.concatenate([main[j, low], cor_n[j], farc_n[j], farc_s[j], cor_s[j], main[j, high]], axis=0)

    _, _, _, _, e2b, n2b, b0 = operator(
        stacked(((fields, low), (row_n, None), (far_n, None), (far_s, None), (row_s, None), (fields, high))),
        strip_band(0), strip_band(1))
    band = [b0]
    for k in range(1, ITERS + 1):
        band.append(step(k, None, band[-1], band[-2] if k > 1 else None, east(band[-1]), north(band[-1]), e2b, n2b))

    def joined(main, halo):
        return jnp.concatenate([main[:rows], halo[HB:2 * HB], halo[4 * HB:5 * HB]], axis=0)

    for k in (ITERS - 1, ITERS):
        up[k % 2] = joined(us[k], band[k])
    for k in range(ITERS + 1, DEG):
        prev, prev2 = up[(k - 1) % 2], up[k % 2]
        le, ln = east(prev), north(prev)
        ue[k - 1], unn[k - 1] = le[:rows, :cols], ln[:rows, :cols]
        x = step(k, None, prev, prev2, le, ln, e2r[...], n2r[...])
        keep(k, x)
        up[k % 2] = x

    wet_in = wet[:rows, :cols]
    me = wet_in * east(wet)[:rows, :cols]
    mn = wet_in * north(wet)[:rows, :cols]
    geo[0], geo[1] = me, mn
    geo[2] = me * rs_e[:rows, :cols]
    geo[3] = mn * rs_n[:rows, :cols]
    geo[4] = rs_in
    rs_z = rsr[:rz, :cols]
    dia[...] = -0.5 * rs_z * rs_z
    rs_c = rsr[:rows, cols:cols + 1]
    us_side[DEG] = to_lanes(-0.5 * rs_c * rs_c)

    def products(t, carry):
        at = pl.ds(pl.multiple_of(t * 8, 8), 8)
        u = [un[k, at, :] for k in range(DEG)]
        for s in range(DEG):
            acc = None
            for a in range((s + 1) // 2):
                pr = u[a] * u[s - a]
                acc = pr if acc is None else acc + pr
            acc = acc + acc if acc is not None else None
            if s % 2 == 0:
                sq = u[s // 2] * u[s // 2]
                acc = sq if acc is None else acc + sq
            ww[s, at, :] = acc
        return carry

    def cross(t, carry):
        at = pl.ds(pl.multiple_of(t * 8, 8), 8)
        for src, dst in ((ue, xe), (unn, xn)):
            for s in range(DEG - 1):
                acc = None
                for a in range(s + 1):
                    pr = un[a, at, :cols] * src[s - a, at, :]
                    acc = pr if acc is None else acc + pr
                dst[s, at, :] = acc
        return carry

    lax.fori_loop(0, rz // 8, products, 0)
    lax.fori_loop(0, rows // 8, cross, 0)

    arrive(range(late, len(groups)))

    for j in range(strips + 2):
        a, b = ((wmain.at[0, j], wmain.at[1, j]) if j < strips else
                (wcor_n.at[0], wcor_n.at[1]) if j == strips else (wcor_s.at[0], wcor_s.at[1]))
        comb[j] = jnp.where(lane8 % GROUP < HW, a[...], b[...])

    def ring_row(r):
        return r if r >= 0 else full + r

    def line(ref, r):
        q = ring_row(r)
        return ref[q:q + 1, :]

    for r in range(-HS, rows + HW):
        if r < 0:
            block, packed, g = wrow_s[r + HS], comb[strips + 1], 8 + r
        elif r >= rows:
            block, packed, g = wrow_n[r - rows], comb[strips], r - rows
        else:
            block, packed, g = w_ref[r], comb[r // 8], r % 8
        side_r = roll(packed, -GROUP * g, 1)
        v[0, r + HS] = line(rsr, r) * jnp.concatenate([block, side_r], axis=1)

    for k in range(1, ITERS):
        for r in range(k - HS, rows + HW - k):
            x = v[k - 1, r + HS]
            e = line(e2r, r)
            le = east(x)
            y = e * le + roll(e * x, 1, 1) + line(n2r, r) * v[k - 1, r + HS + 1] + line(n2r, r - 1) * v[k - 1, r + HS - 1]
            if k > 1:
                before = v[k - 2, r + HS]
                y = y - (before + before if k == 2 else before)
            v[k, r + HS] = y
            if 0 <= r < rows:
                ve[k - 1, r] = le[:, :cols]
    for k in range(ITERS):
        acc = jnp.zeros((costs, 128), jnp.float32)
        for r in range(rows):
            acc = jnp.where(lane8 == r, roll(v[k, r + HS, :, cols:], r, 1), acc)
        vs_side[k] = acc

    total = finish(0, group, mine)
    for stage in range(1, len(stages)):
        total = finish(stage, start(stage, total), total)

    tot8 = jnp.broadcast_to(total, (costs, 128))
    def pick(index):
        return jnp.broadcast_to(
            jnp.sum(jnp.where(lane8 == index, tot8, 0.0), axis=1, keepdims=True), (costs, 128))

    proj = [pick(k * costs + sub8) * (0.5 if k else 1.0) for k in range(ITERS)]
    raw = [pick(mom + m) * (0.5 if m == 1 else 0.25 if m else 1.0) for m in range(DEG)]
    mu = [raw[0], raw[1]]
    for k in range(1, ITERS):
        mu += [2.0 * raw[2 * k] - raw[0], 2.0 * raw[2 * k + 1] - raw[1]]
    c, bar = coefficients(mu, proj)
    zero = jnp.zeros_like(c[0])
    acc = [zero] * (ITERS + 2)
    for m in range(ITERS - 1, -1, -1):
        acc[m] = c[m] + acc[m + 2]
    tail = [zero] * (DEG + 2)
    for m in range(DEG - 1, -1, -1):
        tail[m] = bar[m] + tail[m + 2]
    for m in range(ITERS):
        coef[CS + m] = acc[m]
        coef[CC + m] = 0.5 * c[m] if m else c[m]
    for s in range(DEG - 1):
        coef[CX + s] = 2.0 * tail[s + 1]
    for s in range(DEG):
        coef[CH + s] = tail[s] + tail[s + 2] if s else 2.0 * tail[0]
        coef[CM + s] = bar[s] if s else 2.0 * bar[0]
    sent(range(len(groups)))
    for c in waits:
        c.wait_send()


def adjoint_kernel(un, ue, xe, xn, ww, v, ve, geo, dia, coef, us_side, vs_side,
                   fa_hbm, ge_hbm, gn_hbm, y, ye, z, fa_ref, ge_ref, gn_ref, osem):
    rows, costs, cols = fa_ref.shape
    rz = dia.shape[0]

    outs = ((fa_ref, fa_hbm), (ge_ref, ge_hbm), (gn_ref, gn_hbm))

    def factor(i, width, at=None):
        c = coef[i] if at is None else coef[i, at:at + 1]
        return jnp.concatenate([c] * (width // 128), axis=1)

    def vectors(u, width, at):
        return [total_of(factor(CS + a + b + 1, width, at) * u[b] for b in range(ITERS - 1 - a))
                for a in range(-1, ITERS - 1)]

    def diagonal(ys, u, width, at):
        out = [ys[0] + ys[2] + factor(CC, width, at) * u[0]]
        return out + [ys[a] + ys[a + 2] if a + 2 < len(ys) else ys[a] for a in range(1, ITERS)]

    def combine(t, carry):
        at = pl.ds(pl.multiple_of(t * 8, 8), 8)
        u = [un[k, at, :] for k in range(ITERS)]
        ys = vectors(u, cols, 0)
        for a, f in enumerate(diagonal(ys, u, cols, 0)):
            z[a, at, :] = f
        for a in range(ITERS - 1):
            y[a, at, :] = ys[a + 1]
        return carry

    def combine_east(t, carry):
        at = pl.ds(pl.multiple_of(t * 8, 8), 8)
        u = [ue[k, at, :] for k in range(ITERS - 1)]
        for a in range(ITERS - 1):
            ye[a, at, :] = total_of(factor(CS + a + b + 1, cols, 0) * u[b] for b in range(ITERS - 1 - a))
        return carry

    lax.fori_loop(0, rz // 8, combine, 0)
    lax.fori_loop(0, rows // 8, combine_east, 0)
    u = [us_side[k] for k in range(DEG)]
    zs = diagonal(vectors(u, 128, None), u, 128, None)
    side = total_of(zs[a] * vs_side[a] for a in range(ITERS))
    for s in range(DEG):
        side = side + coef[CH + s] * total_of(u[a] * u[s - a] for a in range(s + 1))
    side = side * us_side[DEG]
    lane_c = lax.broadcasted_iota(jnp.int32, (costs, cols), 1)

    def line(ref, *at):
        return ref[(*at[:-1], pl.ds(at[-1], 1), slice(None))]

    def diag_of(r):
        acc = total_of(line(z, a, r) * v[a, r + HS, :, :cols] for a in range(ITERS))
        for s in range(DEG):
            acc = acc + factor(CH + s, cols) * line(ww, s, r)
        return acc * line(dia, r)

    def rows_of(rs, above):
        def add(acc, term):
            return term if acc is None else acc + term

        ge, gn, fa, db = ([None] * len(rs) for _ in range(4))
        for i, r in enumerate(rs):
            for a in range(ITERS):
                x = v[a, r + HS, :, :cols]
                db[i] = add(db[i], x * line(z, a, r))
                fa[i] = add(fa[i], x * factor(CC + a, cols))
                if a < ITERS - 1:
                    here = line(y, a, r)
                    ge[i] = add(ge[i], x * line(ye, a, r) + ve[a, r] * here)
                    gn[i] = add(gn[i], x * line(y, a, r + 1) + v[a, r + HS + 1, :, :cols] * here)
        for first, count, acc, field in ((CH, DEG, db, ww), (CX, DEG - 1, ge, xe), (CX, DEG - 1, gn, xn), (CM, DEG, fa, un)):
            for s in range(count):
                c = factor(first + s, cols)
                for i, r in enumerate(rs):
                    acc[i] = acc[i] + c * line(field, s, r)
        for i, r in enumerate(rs):
            d = db[i] * line(dia, r)
            end = jnp.concatenate([pltpu.roll(side, 127 - r, 1)] * (cols // 128), axis=1)
            d_e = jnp.where(lane_c == cols - 1, end, east(d))
            fa_ref[r] = line(geo, 4, r) * fa[i]
            ge_ref[r] = line(geo, 2, r) * ge[i] + line(geo, 0, r) * (d + d_e)
            gn_ref[r] = line(geo, 3, r) * gn[i] + line(geo, 1, r) * (d + above)
            above = d
        return above

    last = max(BLOCK, rows // 4 // BLOCK * BLOCK)

    def block(i, above):
        first = rows - (i + 1) * BLOCK
        for j in range(BLOCK - 1, -1, -GROUPED):
            above = rows_of([first + j - i for i in range(GROUPED)], above)
        return above

    above = diag_of(rows)
    for low, high in ((last, rows), (0, last)):
        above = lax.fori_loop((rows - high) // BLOCK, (rows - low) // BLOCK, block, above)
        at = pl.ds(low, high - low)
        for i, (src, dst) in enumerate(outs):
            for n in range(costs):
                pltpu.make_async_copy(src.at[at, n, :], dst.at[n, at], osem.at[i]).start()
    for i, (src, dst) in enumerate(outs):
        pltpu.make_async_copy(dst, dst, osem.at[i]).wait()


def solution(mesh):
    nlat, nlon = mesh.shape["lat"], mesh.shape["lon"]

    def body(forcing, depth_east, depth_north, surface_term, ocean_mask, cost_weights):
        costs, rows, cols = cost_weights.shape
        full, ringc = rows + 2 * HB, cols + 128
        f32 = jnp.float32
        dma = pltpu.SemaphoreType.DMA
        every = [(a, b) for a in range(nlat) for b in range(nlon) if a or b]
        stages = [every] if len(every) < 64 else [
            [(0, b) for b in range(1, nlon)], [(a, 0) for a in range(1, nlat)]]
        reduce_scratch = [
            ref for g in stages for ref in (
                pltpu.VMEM((1, 128), f32), pltpu.VMEM((len(g), 1, 128), f32),
                dma, dma)]
        rz = rows + HB
        shapes = (
            (DEG, rz, cols), (DEG - 1, rows, cols), (DEG - 1, rows, cols), (DEG - 1, rows, cols), (DEG, rz, cols),
            (ITERS, rows + HS + HW, costs, ringc), (ITERS - 1, rows, costs, cols),
            (5, rows, cols), (rz, cols), (NCOEF, costs, 128), (DEG + 1, costs, 128), (ITERS, costs, 128))
        hbm = pl.BlockSpec(memory_space=pltpu.HBM)
        vmem = pl.BlockSpec(memory_space=pltpu.VMEM)
        args = (forcing, depth_east, depth_north, surface_term, ocean_mask, cost_weights)
        mids = pl.pallas_call(
            functools.partial(kernel, nlat, nlon, stages),
            out_shape=[pltpu.VMEM(x, f32) for x in shapes],
            in_specs=[hbm] * 6,
            out_specs=[vmem] * len(shapes),
            scratch_shapes=[
                pltpu.VMEM((5, rows, cols), f32),
                pltpu.VMEM((rows, cols), jnp.int32),
                pltpu.VMEM((rows, costs, cols), f32),
                dma((3,)),
                pltpu.VMEM((rows, 128), f32),
                pltpu.VMEM((rows, 128), f32),
                pltpu.VMEM((2, rows, 128), f32),
                *[pltpu.VMEM((5, HB, cols), f32)] * 2,
                *[pltpu.VMEM((2, HB, 128), f32)] * 2,
                *[pltpu.VMEM((5, HB, cols), f32)] * 2,
                *[pltpu.VMEM((2, HB, 128), f32)] * 2,
                pltpu.VMEM((HW, costs, cols), f32),
                pltpu.VMEM((HS, costs, cols), f32),
                *[pltpu.VMEM((rows // 8, costs, 128), f32)] * 2,
                pltpu.VMEM((2, rows // 8, costs, 128), f32),
                *[pltpu.VMEM((2, costs, 128), f32)] * 2,
                pltpu.VMEM((2, full, ringc), f32),
                pltpu.VMEM((DEG - 1, rows, cols), f32),
                *[pltpu.VMEM((full, ringc), f32)] * 3,
                pltpu.VMEM((rows // 8 + 2, costs, 128), f32),
                dma((14,)),
                dma((14,)),
                pltpu.SemaphoreType.REGULAR((max(1, (max(nlat - 1, nlon // 2) - 1).bit_length()),)),
                *reduce_scratch,
            ],
            compiler_params=pltpu.CompilerParams(
                collective_id=0, has_side_effects=True, vmem_limit_bytes=24 * 1024 * 1024
            ),
        )(*[pltpu.with_memory_space_constraint(x, pltpu.HBM) for x in args])
        out = (costs, rows, cols)
        return pl.pallas_call(
            adjoint_kernel,
            out_shape=[jax.ShapeDtypeStruct(out, f32)] * 3,
            in_specs=[vmem] * len(shapes),
            out_specs=[hbm] * 3,
            scratch_shapes=[
                pltpu.VMEM((ITERS - 1, rz, cols), f32),
                pltpu.VMEM((ITERS - 1, rows, cols), f32),
                pltpu.VMEM((ITERS, rz, cols), f32),
                *[pltpu.VMEM((rows, costs, cols), f32)] * 3,
                dma((3,)),
            ],
            compiler_params=pltpu.CompilerParams(vmem_limit_bytes=24 * 1024 * 1024),
        )(*[pltpu.with_memory_space_constraint(x, pltpu.VMEM) for x in mids])

    grid = P("lat", "lon")
    field = P(None, "lat", "lon")
    return jax.shard_map(
        body,
        mesh=mesh,
        in_specs=(grid, grid, grid, grid, grid, field),
        out_specs=(field, field, field),
        check_vma=False,
    )
```

```python
import functools

import jax
import jax.numpy as jnp
from jax import lax
from jax.experimental import pallas as pl
from jax.experimental.pallas import tpu as pltpu
from jax.sharding import PartitionSpec as P

ITERS = 6
MESH = pl.DeviceIdType.MESH
HB = 8
HS = 5
BLOCK = 8
GROUPED = 4
HC = 13
HW = 6
GROUP = 16
DEG = 2 * ITERS
CS, CC = 0, ITERS
CX = CC + ITERS
CH = CX + DEG - 1
CM = CH + DEG
NCOEF = CM + DEG


def coefficients(mu, proj):
    def gram(a, b):
        return 0.5 * (mu[a + b] + mu[abs(a - b)])

    h = {}
    for a in range(ITERS):
        for b in range(a, ITERS):
            h[a, b] = gram(a, b) - 0.5 * (gram(a, b + 1) + gram(a, abs(b - 1)))
    g, p = list(mu[:ITERS]), list(proj)
    low, inv = {}, []
    for i in range(ITERS):
        inv.append(1.0 / h[i, i])
        for j in range(i + 1, ITERS):
            low[j, i] = h[i, j] * inv[i]
        for j in range(i + 1, ITERS):
            for k in range(j, ITERS):
                h[j, k] = h[j, k] - low[j, i] * h[i, k]
            g[j] = g[j] - low[j, i] * g[i]
            p[j] = p[j] - low[j, i] * p[i]
    c, d = [None] * ITERS, [None] * ITERS
    for i in range(ITERS - 1, -1, -1):
        c[i], d[i] = g[i] * inv[i], p[i] * inv[i]
        for j in range(i + 1, ITERS):
            c[i] = c[i] - low[j, i] * c[j]
            d[i] = d[i] - low[j, i] * d[j]
    zero = jnp.zeros_like(c[0])
    cc = c + [zero, zero]
    res = [1.0 - c[0] + 0.5 * c[1], c[0] + 0.5 * cc[2] - c[1]]
    for j in range(2, ITERS + 1):
        res.append(0.5 * (cc[j - 1] + cc[j + 1]) - cc[j])
    bar = [zero] * DEG
    for a in range(ITERS):
        half = 0.5 * d[a]
        for j in range(ITERS + 1):
            t = half * res[j]
            bar[a + j] = bar[a + j] + t
            bar[abs(a - j)] = bar[abs(a - j)] + t
    return c, bar


def roll(x, shift, axis):
    return pltpu.roll(x, shift % x.shape[axis], axis)


def east(x):
    return roll(x, -1, 1)


def north(x):
    return roll(x, -1, 0)


def total_of(terms):
    acc = None
    for t in terms:
        acc = t if acc is None else acc + t
    return acc


def kernel(nlat, nlon, stages, f_hbm, de_hbm, dn_hbm, st_hbm, mk_hbm, w_hbm,
           un, ue, xe, xn, ww, v, ve, geo, dia, coef, us_side, vs_side,
           fields, mk_ref, w_ref, lsem,
           send_w, send_e, main, row_n, row_s, cor_n, cor_s, far_n, far_s, farc_n, farc_s,
           wrow_n, wrow_s, wsend_w, wsend_e, wmain, wcor_n, wcor_s,
           up, unn, e2r, n2r, rsr, comb, ssem, rsem, hello,
           *reduce_refs):
    lat, lon = lax.axis_index("lat"), lax.axis_index("lon")
    rows, costs, cols = w_ref.shape
    for i, src in enumerate((f_hbm, de_hbm, dn_hbm, st_hbm)):
        pltpu.make_async_copy(src, fields.at[i], lsem.at[0]).start()
    pltpu.make_async_copy(mk_hbm, mk_ref, lsem.at[1]).start()
    for n in range(costs):
        pltpu.make_async_copy(w_hbm.at[n], w_ref.at[:, n, :], lsem.at[2]).start()

    def loaded(i, ref):
        pltpu.make_async_copy(ref, ref, lsem.at[i]).wait()

    def peer(dlat, dlon):
        return (lax.rem(lat + dlat + nlat, nlat), lax.rem(lon + dlon + nlon, nlon))

    has_s, has_n = lat > 0, lat < nlat - 1

    def beside(r):
        return sorted({-r % nlon, 0, r % nlon})

    def greet(sem, r):
        for dlat, there in ((0, None), (-r, lat >= r), (r, lat < nlat - r)):
            def go(dlat=dlat):
                for b in beside(r):
                    if dlat or b:
                        pl.semaphore_signal(sem, inc=1, device_id=(lat + dlat, lax.rem(lon + b, nlon)),
                                            device_id_type=MESH)
            if there is None:
                go()
            elif r < nlat:
                pl.when(there)(go)

    def greeted(sem, r):
        lines = 1 + (lat >= r).astype(jnp.int32) + (lat < nlat - r).astype(jnp.int32)
        pl.semaphore_wait(sem, lines * len(beside(r)) - 1)

    barrier = pltpu.get_barrier_semaphore()
    rounds, radius = [], 1
    while radius < max(nlat - 1, nlon // 2):
        rounds.append(radius)
        radius *= 2
    greet(barrier, 1)

    @pl.when(lat == nlat - 1)
    def _():
        for ref in (row_n, cor_n, far_n, farc_n, wrow_n, wcor_n):
            ref[...] = jnp.zeros_like(ref)

    @pl.when(lat == 0)
    def _():
        for ref in (row_s, cor_s, far_s, farc_s, wrow_s, wcor_s):
            ref[...] = jnp.zeros_like(ref)

    loaded(0, fields.at[pl.ds(0, 4)])
    loaded(1, mk_ref)
    fields[4] = mk_ref[...].astype(jnp.float32)

    lane = lax.broadcasted_iota(jnp.int32, (rows, 128), 1)
    for ref, at, first in ((send_w, slice(0, 128), True), (send_e, slice(cols - 128, cols), False)):
        buf = jnp.zeros((rows, 128), jnp.float32)
        for i in range(5):
            pos = HC * i
            tile = fields[i, :, at]
            tile = roll(tile, pos if first else pos + HC, 1)
            buf = jnp.where((lane >= pos) & (lane < pos + HC), tile, buf)
        ref[...] = buf
    greeted(barrier, 1)
    if rounds:
        greet(hello.at[0], rounds[0])

    groups, pending = [], []

    def whole(i):
        ref = groups[i][0]
        return pltpu.make_async_remote_copy(src_ref=ref, dst_ref=ref, send_sem=ssem.at[groups[i][1] % 3], recv_sem=rsem.at[i],
                                            device_id=peer(0, 1), device_id_type=MESH)

    def send(ref, side, parts):
        i = len(groups)
        groups.append((ref, side))
        pending.append((i, side, parts))

    def depart():
        for i, side, parts in pending:
            def go(i=i, side=side, parts=parts):
                for src, dst, dev in parts:
                    pltpu.make_async_remote_copy(src_ref=src, dst_ref=dst, send_sem=ssem.at[side % 3], recv_sem=rsem.at[i],
                                                 device_id=dev, device_id_type=MESH).start()
            if side == 0:
                go()
            else:
                pl.when(has_s if side > 0 else has_n)(go)
        pending.clear()

    def arrive(span):
        for i in span:
            side = groups[i][1]
            if side == 0:
                whole(i).wait_recv()
            else:
                pl.when(has_n if side > 0 else has_s)(lambda i=i: whole(i).wait_recv())

    def sent(side):
        blocks = sum(ref.size for ref, at in groups if at == side) // (costs * 128)
        ref = coef.at[pl.ds(0, blocks)]
        pltpu.make_async_remote_copy(src_ref=ref, dst_ref=ref, send_sem=ssem.at[side % 3], recv_sem=rsem.at[0],
                                     device_id=peer(0, 1), device_id_type=MESH).wait_send()

    lo, hi, lo2, hi2 = (pl.ds(i, HB) for i in (0, rows - HB, HB, rows - 2 * HB))

    def corners(to, side, at):
        send(to, side, [(send_w.at[at], to.at[0], peer(-side, -1)), (send_e.at[at], to.at[1], peer(-side, 1))])

    corners(cor_n, 1, lo)
    corners(cor_s, -1, hi)
    send(row_n, 1, [(fields.at[:, lo], row_n, peer(-1, 0))])
    send(row_s, -1, [(fields.at[:, hi], row_s, peer(1, 0))])
    send(main, 0, [(send_w, main.at[0], peer(0, -1)), (send_e, main.at[1], peer(0, 1))])
    depart()
    early = len(groups)
    corners(farc_n, 1, lo2)
    corners(farc_s, -1, hi2)
    send(far_n, 1, [(fields.at[:, lo2], far_n, peer(-1, 0))])
    send(far_s, -1, [(fields.at[:, hi2], far_s, peer(1, 0))])
    depart()
    late = len(groups)
    loaded(2, w_ref)
    send(wrow_n, 1, [(w_ref.at[pl.ds(0, HW)], wrow_n, peer(-1, 0))])
    send(wrow_s, -1, [(w_ref.at[pl.ds(rows - HS, HS)], wrow_s, peer(1, 0))])
    depart()
    lane8 = lax.broadcasted_iota(jnp.int32, (costs, 128), 1)
    sub8 = lax.broadcasted_iota(jnp.int32, (costs, 128), 0)
    for j in range(rows // 8):
        to_w, to_e = jnp.zeros((costs, 128), jnp.float32), jnp.zeros((costs, 128), jnp.float32)
        for g in range(8):
            at = GROUP * g
            first, last = w_ref[8 * j + g, :, :128], w_ref[8 * j + g, :, cols - 128:]
            to_w = jnp.where((lane8 >= at) & (lane8 < at + HW), roll(first, at, 1), to_w)
            end = at if g else 128
            to_e = jnp.where((lane8 >= end - HS) & (lane8 < end), roll(last, at, 1), to_e)
        wsend_w[j], wsend_e[j] = to_w, to_e
    strips = rows // 8
    for to, side, j in ((wcor_n, 1, 0), (wcor_s, -1, strips - 1)):
        send(to, side, [(wsend_w.at[j], to.at[0], peer(-side, -1)), (wsend_e.at[j], to.at[1], peer(-side, 1))])
    send(wmain, 0, [(wsend_w, wmain.at[0], peer(0, -1)), (wsend_e, wmain.at[1], peer(0, 1))])
    depart()
    for i in range(1, len(rounds)):
        greeted(hello.at[i - 1], rounds[i - 1])
        greet(hello.at[i], rounds[i])
    arrive(range(early))

    full = rows + 2 * HB
    def operator(mains, got_e, got_w):
        height = got_e.shape[0]
        lane = lax.broadcasted_iota(jnp.int32, (height, 128), 1)

        def padded(i):
            a = roll(got_e, -HC * i, 1)
            b = roll(got_w, 128 - HC - HC * i, 1)
            side = jnp.where(lane < HC, a, jnp.where(lane >= 128 - HC, b, 0.0))
            return jnp.concatenate([mains(i), side], axis=1)

        wet = padded(4)
        ex = padded(1) * wet * east(wet)
        ey = padded(2) * wet * north(wet)
        base = wet * padded(3) + 1.0 - wet
        diag = base + ex + roll(ex, 1, 1) + ey + roll(ey, 1, 0)
        rs = lax.rsqrt(diag)
        rs = rs * (1.5 - 0.5 * diag * rs * rs)
        rs_e, rs_n = rs * east(rs), rs * north(rs)
        return wet, rs, rs_e, rs_n, 2.0 * ex * rs_e, 2.0 * ey * rs_n, rs * padded(0)

    def stacked(order):
        return lambda i: jnp.concatenate([ref[i] if at is None else ref[i, at] for ref, at in order], axis=0)

    def strip(j):
        return jnp.concatenate([main[j], cor_n[j], cor_s[j]], axis=0)

    wet, rs, rs_e, rs_n, e2, n2, u0 = operator(
        stacked(((fields, None), (row_n, None), (row_s, None))), strip(0), strip(1))
    e2r[...], n2r[...], rsr[...] = e2, n2, rs
    rz = rows + HB

    lane_r = lax.broadcasted_iota(jnp.int32, (rows, 128), 1)
    row_r = lax.broadcasted_iota(jnp.int32, (rows, 128), 0)

    def to_lanes(column):
        return jnp.broadcast_to(jnp.sum(jnp.where(lane_r == row_r, column, 0.0), axis=0, keepdims=True), (costs, 128))

    def keep(k, u):
        un[k] = u[:rz, :cols]
        us_side[k] = to_lanes(u[:rows, cols:cols + 1])

    def step(k, x, prev, prev2, le, ln, e2, n2):
        s = e2 * le + roll(e2 * prev, 1, 1) + n2 * ln + roll(n2 * prev, 1, 0)
        return s if k == 1 else s - (prev2 + prev2 if k == 2 else prev2)

    us = [u0]
    for k in range(1, ITERS + 1):
        le, ln = east(us[k - 1]), north(us[k - 1])
        keep(k - 1, us[k - 1])
        ue[k - 1], unn[k - 1] = le[:rows, :cols], ln[:rows, :cols]
        us.append(step(k, None, us[k - 1], us[k - 2] if k > 1 else None, le, ln, e2, n2))
    keep(ITERS, us[ITERS])

    inner = [u[:rows, :cols] for u in us]
    rs_in = rs[:rows, :cols]

    mom = ITERS * costs

    def fold(field):
        return total_of(field[i:i + 8, j:j + 128] for i in range(0, rows, 8) for j in range(0, cols, 128))

    mine = jnp.zeros((costs, 128), jnp.float32)
    for k in range(ITERS):
        for m, field in ((2 * k, inner[k] * inner[k]), (2 * k + 1, inner[k] * inner[k + 1])):
            mine = jnp.where(lane8 == mom + m, jnp.sum(fold(field), axis=1, keepdims=True), mine)
    proj = [None] * ITERS
    for r in range(rows):
        wr = w_ref[r] * rsr[r:r + 1, :cols]
        for k in range(ITERS):
            pr = wr * un[k, r:r + 1, :]
            proj[k] = pr if proj[k] is None else proj[k] + pr
    for k in range(ITERS):
        line = total_of(proj[k][:, j:j + 128] for j in range(0, cols, 128))
        mine = jnp.where(lane8 == costs * k + sub8, jnp.sum(line, axis=1, keepdims=True), mine)
    mine = jnp.sum(mine, axis=0, keepdims=True)

    def start(stage, value):
        mailbox, got, ss, rv = reduce_refs[4 * stage:4 * stage + 4]
        mailbox[...] = value
        for i, (a, b) in enumerate(stages[stage]):
            pltpu.make_async_remote_copy(src_ref=mailbox, dst_ref=got.at[i], send_sem=ss, recv_sem=rv,
                                         device_id=peer(a, b), device_id_type=MESH).start()
        all_of = pltpu.make_async_remote_copy(src_ref=got, dst_ref=got, send_sem=ss, recv_sem=rv,
                                              device_id=peer(0, 1), device_id_type=MESH)
        waits.append(all_of)
        return all_of

    def finish(stage, group, value):
        group.wait_recv()
        got = reduce_refs[4 * stage + 1]
        parts = [value] + [got[i] for i in range(len(stages[stage]))]
        while len(parts) > 1:
            parts = [sum(parts[i:i + 2][1:], parts[i]) for i in range(0, len(parts), 2)]
        return parts[0]

    waits = []
    if rounds:
        greeted(hello.at[len(rounds) - 1], rounds[-1])
    group = start(0, mine)

    arrive(range(early, late))

    low, high = slice(rows - HB, rows), slice(0, HB)

    def strip_band(j):
        return jnp.concatenate([main[j, low], cor_n[j], farc_n[j], farc_s[j], cor_s[j], main[j, high]], axis=0)

    _, _, _, _, e2b, n2b, b0 = operator(
        stacked(((fields, low), (row_n, None), (far_n, None), (far_s, None), (row_s, None), (fields, high))),
        strip_band(0), strip_band(1))
    band = [b0]
    for k in range(1, ITERS + 1):
        band.append(step(k, None, band[-1], band[-2] if k > 1 else None, east(band[-1]), north(band[-1]), e2b, n2b))

    def joined(main, halo):
        return jnp.concatenate([main[:rows], halo[HB:2 * HB], halo[4 * HB:5 * HB]], axis=0)

    for k in (ITERS - 1, ITERS):
        up[k % 2] = joined(us[k], band[k])
    for k in range(ITERS + 1, DEG):
        prev, prev2 = up[(k - 1) % 2], up[k % 2]
        le, ln = east(prev), north(prev)
        ue[k - 1], unn[k - 1] = le[:rows, :cols], ln[:rows, :cols]
        x = step(k, None, prev, prev2, le, ln, e2r[...], n2r[...])
        keep(k, x)
        up[k % 2] = x

    wet_in = wet[:rows, :cols]
    me = wet_in * east(wet)[:rows, :cols]
    mn = wet_in * north(wet)[:rows, :cols]
    geo[0], geo[1] = me, mn
    geo[2] = me * rs_e[:rows, :cols]
    geo[3] = mn * rs_n[:rows, :cols]
    geo[4] = rs_in
    rs_z = rsr[:rz, :cols]
    dia[...] = -0.5 * rs_z * rs_z
    rs_c = rsr[:rows, cols:cols + 1]
    us_side[DEG] = to_lanes(-0.5 * rs_c * rs_c)

    def products(t, carry):
        at = pl.ds(pl.multiple_of(t * 8, 8), 8)
        u = [un[k, at, :] for k in range(DEG)]
        for s in range(DEG):
            acc = None
            for a in range((s + 1) // 2):
                pr = u[a] * u[s - a]
                acc = pr if acc is None else acc + pr
            acc = acc + acc if acc is not None else None
            if s % 2 == 0:
                sq = u[s // 2] * u[s // 2]
                acc = sq if acc is None else acc + sq
            ww[s, at, :] = acc
        return carry

    def cross(t, carry):
        at = pl.ds(pl.multiple_of(t * 8, 8), 8)
        for src, dst in ((ue, xe), (unn, xn)):
            for s in range(DEG - 1):
                acc = None
                for a in range(s + 1):
                    pr = un[a, at, :cols] * src[s - a, at, :]
                    acc = pr if acc is None else acc + pr
                dst[s, at, :] = acc
        return carry

    lax.fori_loop(0, rz // 8, products, 0)
    lax.fori_loop(0, rows // 8, cross, 0)

    arrive(range(late, len(groups)))

    for j in range(strips + 2):
        a, b = ((wmain.at[0, j], wmain.at[1, j]) if j < strips else
                (wcor_n.at[0], wcor_n.at[1]) if j == strips else (wcor_s.at[0], wcor_s.at[1]))
        comb[j] = jnp.where(lane8 % GROUP < HW, a[...], b[...])

    def ring_row(r):
        return r if r >= 0 else full + r

    def line(ref, r):
        q = ring_row(r)
        return ref[q:q + 1, :]

    for r in range(-HS, rows + HW):
        if r < 0:
            block, packed, g = wrow_s[r + HS], comb[strips + 1], 8 + r
        elif r >= rows:
            block, packed, g = wrow_n[r - rows], comb[strips], r - rows
        else:
            block, packed, g = w_ref[r], comb[r // 8], r % 8
        side_r = roll(packed, -GROUP * g, 1)
        v[0, r + HS] = line(rsr, r) * jnp.concatenate([block, side_r], axis=1)

    for k in range(1, ITERS):
        for r in range(k - HS, rows + HW - k):
            x = v[k - 1, r + HS]
            e = line(e2r, r)
            le = east(x)
            y = e * le + roll(e * x, 1, 1) + line(n2r, r) * v[k - 1, r + HS + 1] + line(n2r, r - 1) * v[k - 1, r + HS - 1]
            if k > 1:
                before = v[k - 2, r + HS]
                y = y - (before + before if k == 2 else before)
            v[k, r + HS] = y
            if 0 <= r < rows:
                ve[k - 1, r] = le[:, :cols]
    for k in range(ITERS):
        acc = jnp.zeros((costs, 128), jnp.float32)
        for r in range(rows):
            acc = jnp.where(lane8 == r, roll(v[k, r + HS, :, cols:], r, 1), acc)
        vs_side[k] = acc

    total = finish(0, group, mine)
    for stage in range(1, len(stages)):
        total = finish(stage, start(stage, total), total)

    tot8 = jnp.broadcast_to(total, (costs, 128))
    def pick(index):
        return jnp.broadcast_to(
            jnp.sum(jnp.where(lane8 == index, tot8, 0.0), axis=1, keepdims=True), (costs, 128))

    proj = [pick(k * costs + sub8) * (0.5 if k else 1.0) for k in range(ITERS)]
    raw = [pick(mom + m) * (0.5 if m == 1 else 0.25 if m else 1.0) for m in range(DEG)]
    mu = [raw[0], raw[1]]
    for k in range(1, ITERS):
        mu += [2.0 * raw[2 * k] - raw[0], 2.0 * raw[2 * k + 1] - raw[1]]
    c, bar = coefficients(mu, proj)
    zero = jnp.zeros_like(c[0])
    acc = [zero] * (ITERS + 2)
    for m in range(ITERS - 1, -1, -1):
        acc[m] = c[m] + acc[m + 2]
    tail = [zero] * (DEG + 2)
    for m in range(DEG - 1, -1, -1):
        tail[m] = bar[m] + tail[m + 2]
    for m in range(ITERS):
        coef[CS + m] = acc[m]
        coef[CC + m] = 0.5 * c[m] if m else c[m]
    for s in range(DEG - 1):
        coef[CX + s] = 2.0 * tail[s + 1]
    for s in range(DEG):
        coef[CH + s] = tail[s] + tail[s + 2] if s else 2.0 * tail[0]
        coef[CM + s] = bar[s] if s else 2.0 * bar[0]
    sent(0)
    pl.when(has_s)(lambda: sent(1))
    pl.when(has_n)(lambda: sent(-1))
    for c in waits:
        c.wait_send()


def adjoint_kernel(un, ue, xe, xn, ww, v, ve, geo, dia, coef, us_side, vs_side,
                   fa_hbm, ge_hbm, gn_hbm, y, ye, z, fa_ref, ge_ref, gn_ref, osem):
    rows, costs, cols = fa_ref.shape
    rz = dia.shape[0]

    outs = ((fa_ref, fa_hbm), (ge_ref, ge_hbm), (gn_ref, gn_hbm))

    def factor(i, width, at=None):
        c = coef[i] if at is None else coef[i, at:at + 1]
        return jnp.concatenate([c] * (width // 128), axis=1)

    def vectors(u, width, at):
        return [total_of(factor(CS + a + b + 1, width, at) * u[b] for b in range(ITERS - 1 - a))
                for a in range(-1, ITERS - 1)]

    def diagonal(ys, u, width, at):
        out = [ys[0] + ys[2] + factor(CC, width, at) * u[0]]
        return out + [ys[a] + ys[a + 2] if a + 2 < len(ys) else ys[a] for a in range(1, ITERS)]

    def combine(t, carry):
        at = pl.ds(pl.multiple_of(t * 8, 8), 8)
        u = [un[k, at, :] for k in range(ITERS)]
        ys = vectors(u, cols, 0)
        for a, f in enumerate(diagonal(ys, u, cols, 0)):
            z[a, at, :] = f
        for a in range(ITERS - 1):
            y[a, at, :] = ys[a + 1]
        return carry

    def combine_east(t, carry):
        at = pl.ds(pl.multiple_of(t * 8, 8), 8)
        u = [ue[k, at, :] for k in range(ITERS - 1)]
        for a in range(ITERS - 1):
            ye[a, at, :] = total_of(factor(CS + a + b + 1, cols, 0) * u[b] for b in range(ITERS - 1 - a))
        return carry

    lax.fori_loop(0, rz // 8, combine, 0)
    lax.fori_loop(0, rows // 8, combine_east, 0)
    u = [us_side[k] for k in range(DEG)]
    zs = diagonal(vectors(u, 128, None), u, 128, None)
    side = total_of(zs[a] * vs_side[a] for a in range(ITERS))
    for s in range(DEG):
        side = side + coef[CH + s] * total_of(u[a] * u[s - a] for a in range(s + 1))
    side = side * us_side[DEG]
    lane_c = lax.broadcasted_iota(jnp.int32, (costs, cols), 1)

    def line(ref, *at):
        return ref[(*at[:-1], pl.ds(at[-1], 1), slice(None))]

    def diag_of(r):
        acc = total_of(line(z, a, r) * v[a, r + HS, :, :cols] for a in range(ITERS))
        for s in range(DEG):
            acc = acc + factor(CH + s, cols) * line(ww, s, r)
        return acc * line(dia, r)

    def rows_of(rs, above):
        def add(acc, term):
            return term if acc is None else acc + term

        ge, gn, fa, db = ([None] * len(rs) for _ in range(4))
        for i, r in enumerate(rs):
            for a in range(ITERS):
                x = v[a, r + HS, :, :cols]
                db[i] = add(db[i], x * line(z, a, r))
                fa[i] = add(fa[i], x * factor(CC + a, cols))
                if a < ITERS - 1:
                    here = line(y, a, r)
                    ge[i] = add(ge[i], x * line(ye, a, r) + ve[a, r] * here)
                    gn[i] = add(gn[i], x * line(y, a, r + 1) + v[a, r + HS + 1, :, :cols] * here)
        for first, count, acc, field in ((CH, DEG, db, ww), (CX, DEG - 1, ge, xe), (CX, DEG - 1, gn, xn), (CM, DEG, fa, un)):
            for s in range(count):
                c = factor(first + s, cols)
                for i, r in enumerate(rs):
                    acc[i] = acc[i] + c * line(field, s, r)
        for i, r in enumerate(rs):
            d = db[i] * line(dia, r)
            end = jnp.concatenate([pltpu.roll(side, 127 - r, 1)] * (cols // 128), axis=1)
            d_e = jnp.where(lane_c == cols - 1, end, east(d))
            fa_ref[r] = line(geo, 4, r) * fa[i]
            ge_ref[r] = line(geo, 2, r) * ge[i] + line(geo, 0, r) * (d + d_e)
            gn_ref[r] = line(geo, 3, r) * gn[i] + line(geo, 1, r) * (d + above)
            above = d
        return above

    last = max(BLOCK, rows // 4 // BLOCK * BLOCK)

    def block(i, above):
        first = rows - (i + 1) * BLOCK
        for j in range(BLOCK - 1, -1, -GROUPED):
            above = rows_of([first + j - i for i in range(GROUPED)], above)
        return above

    above = diag_of(rows)
    for low, high in ((last, rows), (0, last)):
        above = lax.fori_loop((rows - high) // BLOCK, (rows - low) // BLOCK, block, above)
        at = pl.ds(low, high - low)
        for i, (src, dst) in enumerate(outs):
            for n in range(costs):
                pltpu.make_async_copy(src.at[at, n, :], dst.at[n, at], osem.at[i]).start()
    for i, (src, dst) in enumerate(outs):
        pltpu.make_async_copy(dst, dst, osem.at[i]).wait()


def solution(mesh):
    nlat, nlon = mesh.shape["lat"], mesh.shape["lon"]

    def body(forcing, depth_east, depth_north, surface_term, ocean_mask, cost_weights):
        costs, rows, cols = cost_weights.shape
        full, ringc = rows + 2 * HB, cols + 128
        f32 = jnp.float32
        dma = pltpu.SemaphoreType.DMA
        every = [(a, b) for a in range(nlat) for b in range(nlon) if a or b]
        stages = [every] if len(every) < 64 else [
            [(0, b) for b in range(1, nlon)], [(a, 0) for a in range(1, nlat)]]
        reduce_scratch = [
            ref for g in stages for ref in (
                pltpu.VMEM((1, 128), f32), pltpu.VMEM((len(g), 1, 128), f32),
                dma, dma)]
        rz = rows + HB
        shapes = (
            (DEG, rz, cols), (DEG - 1, rows, cols), (DEG - 1, rows, cols), (DEG - 1, rows, cols), (DEG, rz, cols),
            (ITERS, rows + HS + HW, costs, ringc), (ITERS - 1, rows, costs, cols),
            (5, rows, cols), (rz, cols), (NCOEF, costs, 128), (DEG + 1, costs, 128), (ITERS, costs, 128))
        hbm = pl.BlockSpec(memory_space=pltpu.HBM)
        vmem = pl.BlockSpec(memory_space=pltpu.VMEM)
        args = (forcing, depth_east, depth_north, surface_term, ocean_mask, cost_weights)
        mids = pl.pallas_call(
            functools.partial(kernel, nlat, nlon, stages),
            out_shape=[pltpu.VMEM(x, f32) for x in shapes],
            in_specs=[hbm] * 6,
            out_specs=[vmem] * len(shapes),
            scratch_shapes=[
                pltpu.VMEM((5, rows, cols), f32),
                pltpu.VMEM((rows, cols), jnp.int32),
                pltpu.VMEM((rows, costs, cols), f32),
                dma((3,)),
                pltpu.VMEM((rows, 128), f32),
                pltpu.VMEM((rows, 128), f32),
                pltpu.VMEM((2, rows, 128), f32),
                *[pltpu.VMEM((5, HB, cols), f32)] * 2,
                *[pltpu.VMEM((2, HB, 128), f32)] * 2,
                *[pltpu.VMEM((5, HB, cols), f32)] * 2,
                *[pltpu.VMEM((2, HB, 128), f32)] * 2,
                pltpu.VMEM((HW, costs, cols), f32),
                pltpu.VMEM((HS, costs, cols), f32),
                *[pltpu.VMEM((rows // 8, costs, 128), f32)] * 2,
                pltpu.VMEM((2, rows // 8, costs, 128), f32),
                *[pltpu.VMEM((2, costs, 128), f32)] * 2,
                pltpu.VMEM((2, full, ringc), f32),
                pltpu.VMEM((DEG - 1, rows, cols), f32),
                *[pltpu.VMEM((full, ringc), f32)] * 3,
                pltpu.VMEM((rows // 8 + 2, costs, 128), f32),
                dma((3,)),
                dma((14,)),
                pltpu.SemaphoreType.REGULAR((max(1, (max(nlat - 1, nlon // 2) - 1).bit_length()),)),
                *reduce_scratch,
            ],
            compiler_params=pltpu.CompilerParams(
                collective_id=0, has_side_effects=True, vmem_limit_bytes=24 * 1024 * 1024
            ),
        )(*[pltpu.with_memory_space_constraint(x, pltpu.HBM) for x in args])
        out = (costs, rows, cols)
        return pl.pallas_call(
            adjoint_kernel,
            out_shape=[jax.ShapeDtypeStruct(out, f32)] * 3,
            in_specs=[vmem] * len(shapes),
            out_specs=[hbm] * 3,
            scratch_shapes=[
                pltpu.VMEM((ITERS - 1, rz, cols), f32),
                pltpu.VMEM((ITERS - 1, rows, cols), f32),
                pltpu.VMEM((ITERS, rz, cols), f32),
                *[pltpu.VMEM((rows, costs, cols), f32)] * 3,
                dma((3,)),
            ],
            compiler_params=pltpu.CompilerParams(vmem_limit_bytes=24 * 1024 * 1024),
        )(*[pltpu.with_memory_space_constraint(x, pltpu.VMEM) for x in mids])

    grid = P("lat", "lon")
    field = P(None, "lat", "lon")
    return jax.shard_map(
        body,
        mesh=mesh,
        in_specs=(grid, grid, grid, grid, grid, field),
        out_specs=(field, field, field),
        check_vma=False,
    )
```
